8 devices in a mesh: dp: 2 (over z, y), tp: 4 (over x, core).
Axes of the slice: x: 2, y: 2, z: 1, core: 2. Of those that a mesh axis runs over, the one named last changes fastest.
Arguments:
- x_in: bfloat16 [256, 4096], P('dp'), parts along dimension 0
- tok_pos: int32 [256], P('dp'), parts along dimension 0
- conv_state: bfloat16 [2, 256, 3, 5632], P(None, 'dp', None, 'tp'), parts along dimension 1
- lru_state: float32 [2, 256, 5632], P(None, 'dp', 'tp'), parts along dimension 1
- k_cache: bfloat16 [256, 1024, 128], P('dp'), parts along dimension 0
- v_cache: bfloat16 [256, 1024, 128], P('dp'), parts along dimension 0
- slot_pos: int32 [256, 1024], P('dp'), parts along dimension 0
- norm_scale: bfloat16 [3, 2, 4096], replicated
- rec_wx: bfloat16 [2, 4096, 5632], P(None, None, 'tp')
- rec_bx: bfloat16 [2, 5632], P(None, 'tp')
- rec_wy: bfloat16 [2, 4096, 5632], P(None, None, 'tp')
- rec_by: bfloat16 [2, 5632], P(None, 'tp')
- conv_w: bfloat16 [2, 4, 5632], P(None, None, 'tp')
- conv_b: bfloat16 [2, 5632], P(None, 'tp')
- gate_wa: bfloat16 [2, 32, 176, 176], P(None, 'tp')
- gate_ba: bfloat16 [2, 5632], P(None, 'tp')
- gate_wi: bfloat16 [2, 32, 176, 176], P(None, 'tp')
- gate_bi: bfloat16 [2, 5632], P(None, 'tp')
- a_param: float32 [2, 5632], P(None, 'tp')
- rec_wout: bfloat16 [2, 5632, 4096], P(None, 'tp')
- rec_bout: bfloat16 [2, 4096], replicated
- attn_wq: bfloat16 [4096, 4096], P(None, 'tp')
- attn_wk: bfloat16 [4096, 128], replicated
- attn_wv: bfloat16 [4096, 128], replicated
- attn_wo: bfloat16 [4096, 4096], P('tp')
- attn_bo: bfloat16 [4096], replicated
- mlp_w1: bfloat16 [3, 4096, 12288], P(None, None, 'tp')
- mlp_b1: bfloat16 [3, 12288], P(None, 'tp')
- mlp_w2: bfloat16 [3, 4096, 12288], P(None, None, 'tp')
- mlp_b2: bfloat16 [3, 12288], P(None, 'tp')
- mlp_wd: bfloat16 [3, 12288, 4096], P(None, 'tp')
- mlp_bd: bfloat16 [3, 4096], replicated
Outputs:
- output 1: bfloat16 [256, 4096], P('dp'), parts along dimension 0
- output 2: bfloat16 [2, 256, 3, 5632], P(None, 'dp', None, 'tp'), parts along dimension 1
- output 3: float32 [2, 256, 5632], P(None, 'dp', 'tp'), parts along dimension 1
- output 4: bfloat16 [256, 1024, 128], P('dp'), parts along dimension 0
- output 5: bfloat16 [256, 1024, 128], P('dp'), parts along dimension 0
- output 6: int32 [256, 1024], P('dp'), parts along dimension 0
There are 2 independent parts. The reference program is written for one: setup_inputs(seed, part) draws one part's arguments, and reference() takes and returns one part's arrays. A program takes and returns all parts, laid end to end along the dimension named above; an argument that names none is the same for every part.
All inputs are finite; a program needn't handle non-finite values.
Results may differ from the reference program's by a relative error of at most 0.02.
Values are sent between devices in bfloat16 or wider.
A program may use at most 1.75 GiB of HBM per device.

```python
import jax
import jax.numpy as jnp
from jax import lax

D = 4096
L = 5632
H = 32
F = 12288
HEAD = 128
WINDOW = 1024
BATCH = 128

ROPE_BASE = 10000.0
NORM_EPS = 1e-6


def draw_positions(key):
    key_kind, key_low, key_mid, key_high, key_old = jax.random.split(key, 5)
    pos_kind = jax.random.permutation(key_kind, jnp.arange(BATCH, dtype=jnp.int32) % 4)
    pos_low = jax.random.randint(key_low, (BATCH,), 1, 8, dtype=jnp.int32)
    pos_mid = jax.random.randint(key_mid, (BATCH,), 8, WINDOW, dtype=jnp.int32)
    pos_high = jax.random.randint(key_high, (BATCH,), WINDOW, 4 * WINDOW, dtype=jnp.int32)
    tok_pos = jnp.where(pos_kind == 0, 0, jnp.where(pos_kind == 1, pos_low, jnp.where(pos_kind == 2, pos_mid, pos_high)))
    old_len = jax.random.randint(key_old, (BATCH,), 0, 4 * WINDOW, dtype=jnp.int32)
    written = jnp.where(tok_pos > 0, tok_pos, old_len)
    slot_ids = jnp.arange(WINDOW, dtype=jnp.int32)
    behind = written[:, None] - 1 - slot_ids[None, :]
    slot_pos = jnp.where(behind >= 0, slot_ids[None, :] + WINDOW * (behind // WINDOW), -1)
    return tok_pos.astype(jnp.int32), slot_pos.astype(jnp.int32)


def normal_draw(key, shape, scale):
    return (jax.random.normal(key, shape, jnp.float32) * scale).astype(jnp.bfloat16)


def setup_inputs(seed: int = 0, part: int = 0) -> dict:
    root_key = jax.random.key(seed)
    part_root, shared_root = jax.random.split(root_key)
    part_keys = jax.random.split(jax.random.fold_in(part_root, part), 8)
    weight_keys = jax.random.split(shared_root, 32)
    tok_pos, slot_pos = draw_positions(part_keys[0])
    v_mean = jax.random.normal(part_keys[6], (BATCH, 1, HEAD), jnp.float32)
    v_noise = jax.random.normal(part_keys[5], (BATCH, WINDOW, HEAD), jnp.float32)
    a_root = jax.random.uniform(weight_keys[11], (2, L), jnp.float32, 0.9, 0.999)
    a_soft = -jnp.log(a_root) / 8.0
    block_width = L // H
    return {
        'x_in': normal_draw(part_keys[1], (BATCH, D), 1.0),
        'tok_pos': tok_pos,
        'conv_state': normal_draw(part_keys[2], (2, BATCH, 3, L), 1.0),
        'lru_state': jax.random.normal(part_keys[3], (2, BATCH, L), jnp.float32) * 0.35,
        'k_cache': normal_draw(part_keys[4], (BATCH, WINDOW, HEAD), 1.0),
        'v_cache': (v_mean + v_noise).astype(jnp.bfloat16),
        'slot_pos': slot_pos,
        'norm_scale': normal_draw(weight_keys[0], (3, 2, D), 0.3),
        'rec_wx': normal_draw(weight_keys[1], (2, D, L), D ** -0.5),
        'rec_bx': normal_draw(weight_keys[2], (2, L), 0.3),
        'rec_wy': normal_draw(weight_keys[3], (2, D, L), D ** -0.5),
        'rec_by': normal_draw(weight_keys[4], (2, L), 0.3),
        'conv_w': normal_draw(weight_keys[5], (2, 4, L), 0.5),
        'conv_b': normal_draw(weight_keys[6], (2, L), 0.3),
        'gate_wa': normal_draw(weight_keys[7], (2, H, block_width, block_width), 2.0 * block_width ** -0.5),
        'gate_ba': normal_draw(weight_keys[8], (2, L), 1.5),
        'gate_wi': normal_draw(weight_keys[9], (2, H, block_width, block_width), block_width ** -0.5),
        'gate_bi': normal_draw(weight_keys[10], (2, L), 0.5),
        'a_param': jnp.log(jnp.expm1(a_soft)),
        'rec_wout': normal_draw(weight_keys[12], (2, L, D), L ** -0.5),
        'rec_bout': normal_draw(weight_keys[13], (2, D), 0.2),
        'attn_wq': normal_draw(weight_keys[14], (D, H * HEAD), D ** -0.5),
        'attn_wk': normal_draw(weight_keys[15], (D, HEAD), D ** -0.5),
        'attn_wv': normal_draw(weight_keys[16], (D, HEAD), D ** -0.5),
        'attn_wo': normal_draw(weight_keys[17], (H * HEAD, D), (H * HEAD) ** -0.5),
        'attn_bo': normal_draw(weight_keys[18], (D,), 0.2),
        'mlp_w1': normal_draw(weight_keys[19], (3, D, F), D ** -0.5),
        'mlp_b1': normal_draw(weight_keys[20], (3, F), 0.3),
        'mlp_w2': normal_draw(weight_keys[21], (3, D, F), D ** -0.5),
        'mlp_b2': normal_draw(weight_keys[22], (3, F), 0.3),
        'mlp_wd': normal_draw(weight_keys[23], (3, F, D), F ** -0.5),
        'mlp_bd': normal_draw(weight_keys[24], (3, D), 0.2),
    }


def rms_norm(residual, scale):
    res_f = residual.astype(jnp.float32)
    mean_sq = jnp.mean(res_f * res_f, axis=-1, keepdims=True)
    return (res_f * lax.rsqrt(mean_sq + NORM_EPS) * (1.0 + scale.astype(jnp.float32))).astype(jnp.bfloat16)


def add_update(residual, update, out_bias):
    return (residual.astype(jnp.float32) + update.astype(jnp.bfloat16).astype(jnp.float32) + out_bias.astype(jnp.float32)).astype(jnp.bfloat16)


def rope_tables(tok_pos, head_dim):
    quarter = head_dim // 4
    inv_freq = ROPE_BASE ** (-jnp.arange(quarter, dtype=jnp.float32) / quarter)
    angles = tok_pos.astype(jnp.float32)[:, None] * inv_freq[None, :]
    return jnp.cos(angles), jnp.sin(angles)


def apply_rope(vectors, cosine, sine):
    quarter = vectors.shape[-1] // 4
    first = vectors[..., :quarter]
    second = vectors[..., quarter:2 * quarter]
    return jnp.concatenate([first * cosine - second * sine, second * cosine + first * sine, vectors[..., 2 * quarter:]], axis=-1)


def mlp_update(normed, w_up, b_up, w_lin, b_lin, w_down):
    gate_pre = jnp.dot(normed, w_up, preferred_element_type=jnp.float32) + b_up.astype(jnp.float32)
    lin_pre = jnp.dot(normed, w_lin, preferred_element_type=jnp.float32) + b_lin.astype(jnp.float32)
    hidden = (jax.nn.gelu(gate_pre, approximate=True) * lin_pre).astype(jnp.bfloat16)
    return jnp.dot(hidden, w_down, preferred_element_type=jnp.float32)


def recurrent_update(normed, tok_pos, conv_prev, lru_prev, rec_wx, rec_bx, rec_wy, rec_by, conv_w, conv_b, gate_wa, gate_ba, gate_wi, gate_bi, a_param, rec_wout):
    n_rows = normed.shape[0]
    n_blocks = gate_wa.shape[0]
    block_width = gate_wa.shape[1]
    x_branch = (jnp.dot(normed, rec_wx, preferred_element_type=jnp.float32) + rec_bx.astype(jnp.float32)).astype(jnp.bfloat16)
    y_branch = jax.nn.gelu(jnp.dot(normed, rec_wy, preferred_element_type=jnp.float32) + rec_by.astype(jnp.float32), approximate=True)
    tap_keep = tok_pos[:, None, None] >= jnp.arange(3, 0, -1, dtype=jnp.int32)[None, :, None]
    history = jnp.where(tap_keep, conv_prev.astype(jnp.float32), 0.0)
    tap_w = conv_w.astype(jnp.float32)
    conv_sum = conv_b.astype(jnp.float32) + tap_w[0] * x_branch.astype(jnp.float32) + jnp.sum(history * tap_w[:0:-1][None], axis=1)
    conv_x = conv_sum.astype(jnp.bfloat16)
    blocks = conv_x.reshape(n_rows, n_blocks, block_width).astype(jnp.float32)
    r_pre = jnp.einsum('bhi,hij->bhj', blocks, gate_wa.astype(jnp.float32)).reshape(n_rows, -1) + gate_ba.astype(jnp.float32)
    i_pre = jnp.einsum('bhi,hij->bhj', blocks, gate_wi.astype(jnp.float32)).reshape(n_rows, -1) + gate_bi.astype(jnp.float32)
    log_a = -8.0 * jax.nn.sigmoid(r_pre) * jax.nn.softplus(a_param)
    decay_gate = jnp.exp(log_a)
    in_scale = jnp.sqrt(1.0 - decay_gate * decay_gate)
    is_reset = (tok_pos == 0)[:, None]
    decay_gate = jnp.where(is_reset, 0.0, decay_gate)
    in_scale = jnp.where(is_reset, 1.0, in_scale)
    lru_new = decay_gate * lru_prev + in_scale * jax.nn.sigmoid(i_pre) * conv_x.astype(jnp.float32)
    gated_h = (lru_new * y_branch).astype(jnp.bfloat16)
    update = jnp.dot(gated_h, rec_wout, preferred_element_type=jnp.float32)
    conv_new = jnp.concatenate([conv_prev[:, 1:], x_branch[:, None, :]], axis=1)
    return update, conv_new, lru_new


def attention_update(normed, tok_pos, k_cache, v_cache, slot_pos, attn_wq, attn_wk, attn_wv, attn_wo):
    n_rows = normed.shape[0]
    head_dim = attn_wk.shape[1]
    window = k_cache.shape[1]
    cosine, sine = rope_tables(tok_pos, head_dim)
    q_heads = jnp.dot(normed, attn_wq, preferred_element_type=jnp.float32).reshape(n_rows, -1, head_dim)
    q_heads = apply_rope(q_heads, cosine[:, None, :], sine[:, None, :]).astype(jnp.bfloat16)
    k_new = apply_rope(jnp.dot(normed, attn_wk, preferred_element_type=jnp.float32), cosine, sine).astype(jnp.bfloat16)
    v_new = jnp.dot(normed, attn_wv, preferred_element_type=jnp.float32).astype(jnp.bfloat16)
    target = jnp.arange(window, dtype=jnp.int32)[None, :] == (tok_pos % window)[:, None]
    k_next = jnp.where(target[:, :, None], k_new[:, None, :], k_cache)
    v_next = jnp.where(target[:, :, None], v_new[:, None, :], v_cache)
    slot_next = jnp.where(target, tok_pos[:, None], slot_pos)
    slot_age = tok_pos[:, None] - slot_next
    slot_valid = (slot_next >= 0) & (slot_age >= 0) & (slot_age < window)

    def attend_row(row_args):
        q_row, k_row, v_row, valid_row = row_args
        scores = jnp.einsum('hd,sd->hs', q_row.astype(jnp.float32), k_row.astype(jnp.float32)) * (head_dim ** -0.5)
        scores = jnp.where(valid_row[None, :], scores, -jnp.inf)
        probs_bf = jax.nn.softmax(scores, axis=-1).astype(jnp.bfloat16)
        return jnp.einsum('hs,sd->hd', probs_bf.astype(jnp.float32), v_row.astype(jnp.float32)).astype(jnp.bfloat16)

    heads_out = lax.map(attend_row, (q_heads, k_next, v_next, slot_valid))
    update = jnp.dot(heads_out.reshape(n_rows, -1), attn_wo, preferred_element_type=jnp.float32)
    return update, k_next, v_next, slot_next


def reference(x_in, tok_pos, conv_state, lru_state, k_cache, v_cache, slot_pos, norm_scale, rec_wx, rec_bx, rec_wy, rec_by, conv_w, conv_b, gate_wa, gate_ba, gate_wi, gate_bi, a_param, rec_wout, rec_bout, attn_wq, attn_wk, attn_wv, attn_wo, attn_bo, mlp_w1, mlp_b1, mlp_w2, mlp_b2, mlp_wd, mlp_bd):
    residual = x_in
    conv_list = []
    lru_list = []
    for layer_idx in range(3):
        normed = rms_norm(residual, norm_scale[layer_idx, 0])
        if layer_idx < 2:
            update, conv_new, lru_new = recurrent_update(normed, tok_pos, conv_state[layer_idx], lru_state[layer_idx], rec_wx[layer_idx], rec_bx[layer_idx], rec_wy[layer_idx], rec_by[layer_idx], conv_w[layer_idx], conv_b[layer_idx], gate_wa[layer_idx], gate_ba[layer_idx], gate_wi[layer_idx], gate_bi[layer_idx], a_param[layer_idx], rec_wout[layer_idx])
            conv_list.append(conv_new)
            lru_list.append(lru_new)
            out_bias = rec_bout[layer_idx]
        else:
            update, k_next, v_next, slot_next = attention_update(normed, tok_pos, k_cache, v_cache, slot_pos, attn_wq, attn_wk, attn_wv, attn_wo)
            out_bias = attn_bo
        residual = add_update(residual, update, out_bias)
        normed = rms_norm(residual, norm_scale[layer_idx, 1])
        update = mlp_update(normed, mlp_w1[layer_idx], mlp_b1[layer_idx], mlp_w2[layer_idx], mlp_b2[layer_idx], mlp_wd[layer_idx])
        residual = add_update(residual, update, mlp_bd[layer_idx])
    return (residual, jnp.stack(conv_list), jnp.stack(lru_list), k_next, v_next, slot_next)
```

```python
import jax
import jax.numpy as jnp
from jax import lax
from jax.experimental import pallas as pl
from jax.experimental.pallas import tpu as pltpu
from jax.sharding import PartitionSpec as P

ROPE_BASE = 10000.0
NORM_EPS = 1e-6
BF = jnp.bfloat16
F32 = jnp.float32
ROWS = 128
D = 4096
TILE = 256
CHUNK = 512
N_CHUNK = D // CHUNK
HALF = ROWS // 2
VMEM_LIMIT = 67043328


class Stream:
    def __init__(self, slots, sems, n_slots):
        self.slots, self.sems, self.n_slots = slots, sems, n_slots
        self.phases = []
        self.total = 0

    def add(self, n, *kinds):
        start = self.total
        self.phases.append((start, n, kinds))
        self.total += n
        return start, kinds

    def slot_of(self, t):
        return lax.rem(t, self.n_slots)

    def copies(self, kind, j, slot):
        return [pltpu.make_async_copy(src, self.slots.at[(slot,) + dst], self.sems.at[slot, i]) for i, (src, dst) in enumerate(kind(j))]

    def start_tile(self, kinds, j, slot):
        n = len(kinds)
        if n == 1:
            for c in self.copies(kinds[0], j, slot):
                c.start()
            return
        for which, kind in enumerate(kinds):
            @pl.when(lax.rem(j, n) == which)
            def _(kind=kind):
                for c in self.copies(kind, lax.div(j, n), slot):
                    c.start()

    def issue(self, t, lo, hi):
        for start, n, kinds in self.phases:
            if start + n <= lo or hi <= start:
                continue

            def go(start=start, kinds=kinds):
                self.start_tile(kinds, t - start, self.slot_of(t))

            if start <= lo and hi <= start + n:
                go()
            else:
                pl.when(jnp.logical_and(t >= start, t < start + n))(go)

    def prime(self):
        first = min(self.n_slots, self.total)
        for start, n, kinds in self.phases:
            stop = min(start + n, first)
            if start < stop:
                @pl.loop(start, stop)
                def _(t, start=start, kinds=kinds):
                    self.start_tile(kinds, t - start, self.slot_of(t))

    def wait(self, phase, j):
        start, kinds = phase
        slot = self.slot_of(start + j)
        for c in self.copies(kinds[0], lax.div(j, len(kinds)), slot):
            c.wait()
        return slot


def full(slot_rows):
    return (pl.ds(0, slot_rows), pl.ds(0, TILE))


def columns(ref, layer, rows):
    return lambda j: [(ref.at[layer, :, pl.ds(pl.multiple_of(j * TILE, TILE), TILE)], full(rows))]


def gelu(v):
    return jax.nn.gelu(v, approximate=True)


def f32(v):
    return v.astype(F32)


def cols(k, width=CHUNK):
    return pl.ds(pl.multiple_of(k * width, width), width)


class Comm:
    def __init__(self, part, r1, cs, r2, fin, r3, s1, q1, s2, q2, s3, q3):
        self.part, self.r1, self.cs, self.r2, self.fin, self.r3 = part, r1, cs, r2, fin, r3
        self.s1, self.q1, self.s2, self.q2, self.s3, self.q3 = s1, q1, s2, q2, s3, q3
        me = lax.axis_index('tp')
        self.mine = lax.rem(me, 2)
        self.other = 1 - self.mine
        self.partner = me + 1 - 2 * self.mine
        self.peer = lax.rem(me + 2, 4)

    def barrier(self):
        sem = pltpu.get_barrier_semaphore()
        for dev in (self.partner, self.peer):
            pl.semaphore_signal(sem, inc=1, device_id={'tp': dev}, device_id_type=pl.DeviceIdType.MESH)
        pl.semaphore_wait(sem, 2)

    def copy1(self, par, k):
        return pltpu.make_async_remote_copy(src_ref=self.part.at[k, self.other], dst_ref=self.r1.at[k], send_sem=self.s1.at[par, k], recv_sem=self.q1.at[par, k], device_id={'tp': self.partner}, device_id_type=pl.DeviceIdType.MESH)

    def copy2(self, par, k):
        return pltpu.make_async_remote_copy(src_ref=self.cs.at[k], dst_ref=self.r2.at[par, k], send_sem=self.s2.at[par, k], recv_sem=self.q2.at[par, k], device_id={'tp': self.peer}, device_id_type=pl.DeviceIdType.MESH)

    def copy3(self, par, k):
        return pltpu.make_async_remote_copy(src_ref=self.fin.at[k], dst_ref=self.r3.at[k], send_sem=self.s3.at[par, k], recv_sem=self.q3.at[par, k], device_id={'tp': self.partner}, device_id_type=pl.DeviceIdType.MESH)

    def chip_sum(self, par, k):
        self.copy1(par, k).wait_recv()
        self.cs[k] = (f32(self.part[k, self.mine]) + f32(self.r1[k])).astype(BF)
        self.copy2(par, k).start()

    def finish(self, par, update):
        @pl.loop(0, N_CHUNK)
        def _(k):
            self.copy2(par, k).wait_recv()
            total = (f32(self.cs[k]) + f32(self.r2[par, k])).astype(BF)
            self.fin[k] = total
            self.copy3(par, k).start()
            update(self.mine, k, f32(total))

            @pl.when(k >= 1)
            def _():
                self.copy3(par, k - 1).wait_recv()
                update(self.other, k - 1, f32(self.r3[k - 1]))

        self.copy3(par, N_CHUNK - 1).wait_recv()
        update(self.other, N_CHUNK - 1, f32(self.r3[N_CHUNK - 1]))

        @pl.loop(0, N_CHUNK)
        def _(k):
            self.copy1(par, k).wait_send()
            self.copy2(par, k).wait_send()
            self.copy3(par, k).wait_send()


def fold_lanes(v):
    acc = v[:, 0:128]
    for i in range(1, v.shape[1] // 128):
        acc = acc + v[:, 128 * i:128 * (i + 1)]
    return acc


class Body:
    def __init__(self, stream, comm, x, n, hid, ss, nscale):
        self.stream, self.comm, self.x, self.n, self.hid, self.ss, self.nscale = stream, comm, x, n, hid, ss, nscale
        self.n_ar = 0

    def squares(self):
        self.ss[...] = jnp.zeros_like(self.ss)

        @pl.loop(0, N_CHUNK)
        def _(k):
            v = f32(self.x[:, cols(k)])
            self.ss[...] += fold_lanes(v * v)

    def norm(self, row):
        scale = lax.rsqrt(jnp.sum(self.ss[...], axis=-1, keepdims=True) * (1.0 / D) + NORM_EPS)

        @pl.loop(0, N_CHUNK)
        def _(k):
            gain = 1.0 + f32(self.nscale[row:row + 1, cols(k)])
            self.n[:, cols(k)] = (f32(self.x[:, cols(k)]) * scale * gain).astype(BF)

    def updater(self, bias, row):
        def update(half, k, u):
            rows = pl.ds(pl.multiple_of(half * HALF, HALF), HALF)
            new = (f32(self.x[rows, cols(k)]) + u + f32(bias[row:row + 1, cols(k)])).astype(BF)
            self.x[rows, cols(k)] = new
            v = f32(new)
            self.ss[rows, :] += fold_lanes(v * v)

        return update

    def all_reduce(self, bias, row):
        par = self.n_ar % 2
        self.n_ar += 1
        self.ss[...] = jnp.zeros_like(self.ss)
        self.comm.finish(par, self.updater(bias, row))

    def down(self, phase, depth, per_chunk, lhs):
        st, comm, par = self.stream, self.comm, self.n_ar % 2
        start = phase[0]
        ahead = start + st.n_slots
        stop = ahead + per_chunk * N_CHUNK

        @pl.loop(0, N_CHUNK)
        def _(k):
            for h in range(2):
                if per_chunk == 2 or h == 0:
                    slot = st.wait(phase, k * per_chunk + h)
                off = 0 if per_chunk == 2 else h * depth
                prod = jnp.dot(lhs[...], st.slots[slot, off:off + depth, :], preferred_element_type=F32).astype(BF)
                for r in range(2):
                    comm.part[k, r, :, h * TILE:(h + 1) * TILE] = prod[r * HALF:(r + 1) * HALF]
            for h in range(per_chunk):
                st.issue(ahead + k * per_chunk + h, ahead, stop)
            comm.copy1(par, k).start()

            @pl.when(k >= 1)
            def _():
                comm.chip_sum(par, k - 1)

        comm.chip_sum(par, N_CHUNK - 1)

    def mlp(self, up, down, layer, b1, b2, bd):
        st = self.stream
        start = up[0]
        ahead = start + st.n_slots
        stop = ahead + 24

        @pl.loop(0, 12)
        def _(i):
            s0 = st.wait(up, 2 * i)
            s1 = st.wait(up, 2 * i + 1)
            g = jnp.dot(self.n[...], st.slots[s0], preferred_element_type=F32)
            v = jnp.dot(self.n[...], st.slots[s1], preferred_element_type=F32)
            st.issue(ahead + 2 * i, ahead, stop)
            st.issue(ahead + 2 * i + 1, ahead, stop)
            g = g + f32(b1[layer:layer + 1, cols(i, TILE)])
            v = v + f32(b2[layer:layer + 1, cols(i, TILE)])
            self.hid[:, cols(i, TILE)] = (gelu(g) * v).astype(BF)

        self.down(down, 3072, 2, self.hid)
        self.all_reduce(bd, layer)


    def recurrent(self, x_tiles, mixed, y_tiles, out_tiles, layer, v, outs):
        st = self.stream
        ahead = x_tiles[0] + st.n_slots
        stop = ahead + 11

        @pl.loop(0, 5)
        def _(i):
            slot = st.wait(x_tiles, i)
            g = jnp.dot(self.n[...], st.slots[slot], preferred_element_type=F32)
            st.issue(ahead + i, ahead, stop)
            v.xb[:, cols(i, TILE)] = (g + f32(v.bx[layer:layer + 1, cols(i, TILE)])).astype(BF)

        slot = st.wait(mixed, 0)
        g = jnp.dot(self.n[...], st.slots[slot], preferred_element_type=F32)
        st.issue(ahead + 5, ahead, stop)
        v.xb[:, 1280:1408] = (g[:, 0:128] + f32(v.bx[layer:layer + 1, 1280:1408])).astype(BF)
        v.yg[:, 1280:1408] = gelu(g[:, 128:256] + f32(v.by[layer:layer + 1, 1280:1408]))

        outs.wait_inputs(layer)
        pos = v.tokc[...]

        @pl.loop(0, 11)
        def _(i):
            c = cols(i, 128)
            acc = f32(v.cb[layer:layer + 1, c]) + f32(v.cw[layer, 0:1, c]) * f32(v.xb[:, c])
            for j in range(3):
                acc = acc + jnp.where(pos >= 3 - j, f32(v.conv[layer, j, :, c]), 0.0) * f32(v.cw[layer, 3 - j:4 - j, c])
            v.xc[:, c] = acc.astype(BF)

        for b in range(8):
            c = slice(176 * b, 176 * (b + 1))
            xc = v.xc[:, c]
            v.rp[:, c] = jnp.dot(xc, v.ga[layer, b], preferred_element_type=F32)
            v.ip[:, c] = jnp.dot(xc, v.gi[layer, b], preferred_element_type=F32)

        def gate(c, reset):
            rate = -8.0 * jax.nn.softplus(v.ap[layer:layer + 1, c])
            decay = jnp.exp(rate * jax.nn.sigmoid(v.rp[:, c] + f32(v.gba[layer:layer + 1, c])))
            into = jnp.sqrt(1.0 - decay * decay)
            decay = jnp.where(reset, 0.0, decay)
            into = jnp.where(reset, 1.0, into)
            new = decay * v.lru[layer, :, c] + into * jax.nn.sigmoid(v.ip[:, c] + f32(v.gbi[layer:layer + 1, c])) * f32(v.xc[:, c])
            v.lru[layer, :, c] = new
            return new

        @pl.loop(0, 5)
        def _(i):
            slot = st.wait(y_tiles, i)
            g = jnp.dot(self.n[...], st.slots[slot], preferred_element_type=F32)
            st.issue(ahead + 6 + i, ahead, stop)
            for h in range(2):
                c = cols(2 * i + h, 128)
                new = gate(c, pos == 0)
                y = gelu(g[:, 128 * h:128 * (h + 1)] + f32(v.by[layer:layer + 1, c]))
                v.gated[:, c] = (new * y).astype(BF)

        c = slice(1280, 1408)
        v.gated[:, c] = (gate(c, pos == 0) * v.yg[:, c]).astype(BF)
        outs.write(layer)
        self.down(out_tiles, 1408, 1, v.gated)
        self.all_reduce(v.bout, layer)
        outs.wait_write(layer)


def add_mlp(stream, w1, w2, wd, layer):
    up = stream.add(24, columns(w1, layer, D), columns(w2, layer, D))
    return up, stream.add(16, columns(wd, layer, 3072))


class Names:
    def __init__(self, **kw):
        self.__dict__.update(kw)


class StateCopies:
    def __init__(self, ins, conv_out, lru_out, v, in_sem, out_sem):
        self.ins, self.conv_out, self.lru_out, self.v, self.in_sem, self.out_sem = ins, conv_out, lru_out, v, in_sem, out_sem

    def inputs(self, layer):
        return [pltpu.make_async_copy(src.at[layer], dst.at[layer], self.in_sem.at[layer, i]) for i, (src, dst) in enumerate(self.ins)]

    def start_inputs(self, layer):
        for c in self.inputs(layer):
            c.start()

    def wait_inputs(self, layer):
        for c in self.inputs(layer):
            c.wait()

    def outputs(self, layer):
        pairs = [(self.v.conv.at[layer, pl.ds(1, 2)], self.conv_out.at[layer, pl.ds(0, 2)]), (self.v.xb, self.conv_out.at[layer, 2]), (self.v.lru.at[layer], self.lru_out.at[layer])]
        return [pltpu.make_async_copy(src, dst, self.out_sem.at[layer, i]) for i, (src, dst) in enumerate(pairs)]

    def write(self, layer):
        for c in self.outputs(layer):
            c.start()

    def wait_write(self, layer):
        for c in self.outputs(layer):
            c.wait()


N_SLOTS_A = 21
N_SLOTS_B = 24
N_SLOTS_C = 26

COMM_SCRATCH = [
    pltpu.VMEM((N_CHUNK, 2, HALF, CHUNK), BF), pltpu.VMEM((N_CHUNK, HALF, CHUNK), BF), pltpu.VMEM((N_CHUNK, HALF, CHUNK), BF),
    pltpu.VMEM((2, N_CHUNK, HALF, CHUNK), BF), pltpu.VMEM((N_CHUNK, HALF, CHUNK), BF), pltpu.VMEM((N_CHUNK, HALF, CHUNK), BF),
] + [pltpu.SemaphoreType.DMA((2, N_CHUNK)) for _ in range(6)]


def body_scratch(n_slots, n_pieces):
    return [pltpu.VMEM((n_slots, D, TILE), BF), pltpu.SemaphoreType.DMA((n_slots, n_pieces)), pltpu.VMEM((ROWS, D), BF), pltpu.VMEM((ROWS, D), BF)]


def recurrent_kernel(tok, x_in, conv, lru, nscale, wx, bx, wy, by, cw, cb, ga, gba, gi, gbi, ap, wout, bout, w1, b1, w2, b2, wd, bd, *refs):
    x_out, conv_out, lru_out = refs[:3]
    slots, sems, x, n, hid, ss = refs[3:9]
    comm = Comm(*refs[9:21])
    small = refs[21:35]
    v_tok, v_ns, v_bx, v_by, v_cw, v_cb, v_gba, v_gbi, v_ap, v_bout, v_b1, v_b2, v_bd, small_sem = small
    v_conv, v_lru, v_ga, v_gi, xb, yg, xc, rp, ip, gated, tokc, in_sem, out_sem = refs[35:]
    stream = Stream(slots, sems, N_SLOTS_A)
    v = Names(bx=v_bx, by=v_by, cw=v_cw, cb=v_cb, ga=v_ga, gba=v_gba, gi=v_gi, gbi=v_gbi, ap=v_ap, bout=v_bout, conv=v_conv, lru=v_lru, xb=xb, yg=yg, xc=xc, rp=rp, ip=ip, gated=gated, tokc=tokc)
    outs = StateCopies([(conv, v_conv), (lru, v_lru), (ga, v_ga), (gi, v_gi)], conv_out, lru_out, v, in_sem, out_sem)
    body = Body(stream, comm, x, n, hid, ss, v_ns)

    plan = []
    for layer in range(2):
        xt = stream.add(5, columns(wx, layer, D))
        mixed = stream.add(1, lambda j, layer=layer: [(wx.at[layer, :, 1280:1408], (pl.ds(0, D), pl.ds(0, 128))), (wy.at[layer, :, 1280:1408], (pl.ds(0, D), pl.ds(128, 128)))])
        yt = stream.add(5, columns(wy, layer, D))
        ot = stream.add(8, lambda j, layer=layer: [(wout.at[layer, :, pl.ds(pl.multiple_of(j * CHUNK + h * TILE, TILE), TILE)], (pl.ds(h * 1408, 1408), pl.ds(0, TILE))) for h in range(2)])
        up, down = add_mlp(stream, w1, w2, wd, layer)
        plan.append((xt, mixed, yt, ot, up, down))

    pairs = [(x_in, x), (tok, v_tok), (nscale, v_ns), (bx, v_bx), (by, v_by), (cw, v_cw), (cb, v_cb), (gba, v_gba), (gbi, v_gbi), (ap, v_ap), (bout, v_bout), (b1, v_b1), (b2, v_b2), (bd, v_bd)]
    early = [pltpu.make_async_copy(s, d, small_sem.at[i]) for i, (s, d) in enumerate(pairs)]
    for c in early:
        c.start()
    stream.prime()
    outs.start_inputs(0)
    outs.start_inputs(1)
    comm.barrier()
    for c in early:
        c.wait()
    tokc[...] = jnp.broadcast_to(v_tok[...], (ROWS, 128)).T
    body.squares()
    for layer in range(2):
        xt, mixed, yt, ot, up, down = plan[layer]
        body.norm(2 * layer)
        body.recurrent(xt, mixed, yt, ot, layer, v, outs)
        body.norm(2 * layer + 1)
        body.mlp(up, down, layer, v_b1, v_b2, v_bd)
    last = pltpu.make_async_copy(x, x_out, small_sem.at[0])
    last.start()
    last.wait()


def final_kernel(x_in, part_in, nscale, bo, w1, b1, w2, b2, wd, bd, *refs):
    x_out = refs[0]
    slots, sems, x, n, hid, ss = refs[1:7]
    comm = Comm(*refs[7:19])
    v_ns, v_bo, v_b1, v_b2, v_bd, small_sem = refs[19:]
    stream = Stream(slots, sems, N_SLOTS_C)
    body = Body(stream, comm, x, n, hid, ss, v_ns)
    up, down = add_mlp(stream, w1, w2, wd, 2)
    pairs = [(part_in, comm.part), (x_in, x), (nscale, v_ns), (bo, v_bo), (b1, v_b1), (b2, v_b2), (bd, v_bd)]
    early = [pltpu.make_async_copy(s, d, small_sem.at[i]) for i, (s, d) in enumerate(pairs)]
    for c in early:
        c.start()
    stream.prime()
    comm.barrier()
    for c in early:
        c.wait()

    @pl.loop(0, N_CHUNK)
    def _(k):
        comm.copy1(0, k).start()

    @pl.loop(0, N_CHUNK)
    def _(k):
        comm.chip_sum(0, k)

    body.all_reduce(v_bo, 0)
    body.norm(5)
    body.mlp(up, down, 2, v_b1, v_b2, v_bd)
    last = pltpu.make_async_copy(x, x_out, small_sem.at[0])
    last.start()
    last.wait()


GROUP = 4
N_GROUP = ROWS // GROUP
WINDOW = 1024
HEADS = 8
LAG = 3


def attention_kernel(pos_s, tok, x_in, nscale, cosine, sine, k_cache, v_cache, slot_pos, wq, wk, wv, wo, part_out, k_out, v_out, slot_out,
                     slots, sems, x, n, ss, v_ns, v_tok, v_cos, v_sin, v_slot, bias, tokc, q3, o3, k_new, v_new, o_bf, part, small_sem, out_sem, slot_sem):
    stream = Stream(slots, sems, N_SLOTS_B)
    body = Body(stream, None, x, n, None, ss, v_ns)
    qt = stream.add(4, lambda j: [(wq.at[:, cols(j, TILE)], full(D))])
    kvt = stream.add(1, lambda j: [(wk, (pl.ds(0, D), pl.ds(0, 128))), (wv, (pl.ds(0, D), pl.ds(128, 128)))])

    def group_rows(j):
        return pl.ds(pl.multiple_of(j * GROUP * WINDOW, GROUP * WINDOW), GROUP * WINDOW)

    ct = stream.add(N_GROUP, lambda j: [(src.at[group_rows(j)], (pl.ds(0, D), pl.ds(128 * i, 128))) for i, src in enumerate((k_cache, v_cache))])
    ot = stream.add(4, lambda j: [(wo.at[:, cols(4 * j + h, TILE)], (pl.ds(1024 * h, 1024), pl.ds(0, TILE))) for h in range(4)])

    pairs = [(x_in, x), (tok, v_tok), (nscale, v_ns), (cosine, v_cos), (sine, v_sin), (slot_pos, v_slot)]
    early = [pltpu.make_async_copy(s, d, small_sem.at[i]) for i, (s, d) in enumerate(pairs)]
    for c in early:
        c.start()
    stream.prime()
    for c in early:
        c.wait()
    tokc[...] = jnp.broadcast_to(v_tok[...], (ROWS, 128)).T
    body.squares()
    body.norm(4)

    pos = tokc[...]
    target = lax.rem(pos, WINDOW)

    @pl.loop(0, WINDOW // 128)
    def _(i):
        lane = lax.broadcasted_iota(jnp.int32, (ROWS, 128), 1) + i * 128
        now = jnp.where(lane == target, pos, v_slot[:, cols(i, 128)])
        v_slot[:, cols(i, 128)] = now
        age = pos - now
        good = (now >= 0) & (age >= 0) & (age < WINDOW)
        bias[:, cols(i, 128)] = jnp.where(good, 0.0, -jnp.inf)

    slot_copy = pltpu.make_async_copy(v_slot, slot_out, slot_sem)
    slot_copy.start()

    lane = lax.broadcasted_iota(jnp.int32, (ROWS, 128), 1)

    def rope(val):
        other = jnp.where(lane < 32, pltpu.roll(val, 96, 1), pltpu.roll(val, 32, 1))
        return val * v_cos[...] + other * v_sin[...]

    ahead = stream.n_slots
    for j in range(4):
        slot = stream.wait(qt, j)
        g = jnp.dot(n[...], slots[slot], preferred_element_type=F32)
        stream.issue(ahead + j, ahead, ahead + 5)
        for h in range(2):
            q3[pl.ds(2 * j + h, ROWS, stride=HEADS), :] = f32(rope(g[:, 128 * h:128 * (h + 1)]).astype(BF))
    slot = stream.wait(kvt, 0)
    g = jnp.dot(n[...], slots[slot], preferred_element_type=F32)
    stream.issue(ahead + 4, ahead, ahead + 5)
    k_new[...] = f32(rope(g[:, 0:128]).astype(BF))
    v_new[...] = f32(g[:, 128:256].astype(BF))

    def outputs(j):
        slot = stream.slot_of(ct[0] + j)
        return [pltpu.make_async_copy(slots.at[slot, :, pl.ds(128 * i, 128)], dst.at[group_rows(j)], out_sem.at[slot, i]) for i, dst in enumerate((k_out, v_out))]

    row16 = lax.broadcasted_iota(jnp.int32, (16, 128), 0)
    ahead = ct[0] - LAG + stream.n_slots

    @pl.loop(0, N_GROUP)
    def _(j):
        slot = stream.wait(ct, j)
        for r in range(GROUP):
            seq = j * GROUP + r
            spot = lax.rem(pos_s[seq], WINDOW)
            base = pl.multiple_of(r * WINDOW + lax.div(spot, 16) * 16, 16)
            for i, new in enumerate((k_new, v_new)):
                here = (slot, pl.ds(base, 16), pl.ds(128 * i, 128))
                slots[here] = jnp.where(row16 == lax.rem(spot, 16), new[pl.ds(seq, 1), :], f32(slots[here])).astype(BF)
        for c in outputs(j):
            c.start()
        for r in range(GROUP):
            seq = j * GROUP + r
            q = q3[pl.ds(pl.multiple_of(seq * HEADS, HEADS), HEADS), :].astype(BF)
            keys = slots[slot, r * WINDOW:(r + 1) * WINDOW, 0:128]
            score = lax.dot_general(q, keys, (((1,), (1,)), ((), ())), preferred_element_type=F32) * (128 ** -0.5)
            score = score + bias[pl.ds(seq, 1), :]
            p = jnp.exp(score - jnp.max(score, axis=-1, keepdims=True))
            p = (p / jnp.sum(p, axis=-1, keepdims=True)).astype(BF)
            o = jnp.dot(p, slots[slot, r * WINDOW:(r + 1) * WINDOW, 128:256], preferred_element_type=F32)
            o3[pl.ds(pl.multiple_of(seq * HEADS, HEADS), HEADS), :] = o

        @pl.when(j >= LAG)
        def _():
            for c in outputs(j - LAG):
                c.wait()
            stream.issue(ahead + j, ahead + LAG, ahead + N_GROUP)

    for h in range(HEADS):
        o_bf[:, 128 * h:128 * (h + 1)] = o3[pl.ds(h, ROWS, stride=HEADS), :].astype(BF)

    @pl.loop(0, 4)
    def _(j):
        slot = stream.wait(ot, j)
        for h in range(4):
            prod = jnp.dot(o_bf[...], slots[slot, 1024 * h:1024 * (h + 1), :], preferred_element_type=F32).astype(BF)
            for r in range(2):
                part[2 * j + h // 2, r, :, (h % 2) * TILE:(h % 2 + 1) * TILE] = prod[r * HALF:(r + 1) * HALF]

    last = pltpu.make_async_copy(part, part_out, small_sem.at[0])
    last.start()
    for j in range(N_GROUP - LAG, N_GROUP):
        for c in outputs(j):
            c.wait()
    slot_copy.wait()
    last.wait()


ANY = pl.BlockSpec(memory_space=pl.ANY)


def rope_tables(tok_pos):
    quarter = 32
    inv_freq = ROPE_BASE ** (-jnp.arange(quarter, dtype=F32) / quarter)
    angles = tok_pos.astype(F32)[:, None] * inv_freq[None, :]
    cosine, sine = jnp.cos(angles), jnp.sin(angles)
    rows = tok_pos.shape[0]
    return (jnp.concatenate([cosine, cosine, jnp.ones((rows, 64), F32)], axis=1), jnp.concatenate([-sine, sine, jnp.zeros((rows, 64), F32)], axis=1))


def io_specs():
    in_specs = (P('dp', None), P('dp'), P(None, 'dp', None, 'tp'), P(None, 'dp', 'tp'), P('dp', None, None), P('dp', None, None), P('dp', None),
                P(), P(None, None, 'tp'), P(None, 'tp'), P(None, None, 'tp'), P(None, 'tp'), P(None, None, 'tp'), P(None, 'tp'),
                P(None, 'tp', None, None), P(None, 'tp'), P(None, 'tp', None, None), P(None, 'tp'), P(None, 'tp'), P(None, 'tp', None), P(),
                P(None, 'tp'), P(), P(), P('tp', None), P(),
                P(None, None, 'tp'), P(None, 'tp'), P(None, None, 'tp'), P(None, 'tp'), P(None, 'tp', None), P())
    out_specs = (P('dp', None), P(None, 'dp', None, 'tp'), P(None, 'dp', 'tp'), P('dp', None, None), P('dp', None, None), P('dp', None))
    return in_specs, out_specs


def solution(mesh):
    in_specs, out_specs = io_specs()
    shape = jax.ShapeDtypeStruct

    def local_step(x_in, tok_pos, conv_state, lru_state, k_cache, v_cache, slot_pos, norm_scale, rec_wx, rec_bx, rec_wy, rec_by, conv_w, conv_b, gate_wa, gate_ba, gate_wi, gate_bi, a_param, rec_wout, rec_bout, attn_wq, attn_wk, attn_wv, attn_wo, attn_bo, mlp_w1, mlp_b1, mlp_w2, mlp_b2, mlp_wd, mlp_bd):
        tok = tok_pos.reshape(1, ROWS)
        scales = norm_scale.reshape(6, D)
        cosine, sine = rope_tables(tok_pos)
        vec = pltpu.VMEM((2, 1408), BF)
        x_mid, conv_out, lru_out = pl.pallas_call(
            recurrent_kernel,
            out_shape=[shape((ROWS, D), BF), shape((2, 3, ROWS, 1408), BF), shape((2, ROWS, 1408), F32)],
            in_specs=[ANY] * 24, out_specs=[ANY] * 3,
            scratch_shapes=body_scratch(N_SLOTS_A, 2) + [pltpu.VMEM((ROWS, 3072), BF), pltpu.VMEM((ROWS, 128), F32)] + COMM_SCRATCH + [
                pltpu.VMEM((1, ROWS), jnp.int32), pltpu.VMEM((6, D), BF), vec, vec, pltpu.VMEM((2, 4, 1408), BF), vec, vec, vec, pltpu.VMEM((2, 1408), F32),
                pltpu.VMEM((2, D), BF), pltpu.VMEM((3, 3072), BF), pltpu.VMEM((3, 3072), BF), pltpu.VMEM((3, D), BF), pltpu.SemaphoreType.DMA((14,)),
                pltpu.VMEM((2, 3, ROWS, 1408), BF), pltpu.VMEM((2, ROWS, 1408), F32), pltpu.VMEM((2, 8, 176, 176), BF), pltpu.VMEM((2, 8, 176, 176), BF),
                pltpu.VMEM((ROWS, 1408), BF), pltpu.VMEM((ROWS, 1408), F32), pltpu.VMEM((ROWS, 1408), BF), pltpu.VMEM((ROWS, 1408), F32), pltpu.VMEM((ROWS, 1408), F32),
                pltpu.VMEM((ROWS, 1408), BF), pltpu.VMEM((ROWS, 128), jnp.int32), pltpu.SemaphoreType.DMA((2, 4)), pltpu.SemaphoreType.DMA((2, 3))],
            compiler_params=pltpu.CompilerParams(collective_id=0, has_side_effects=True, vmem_limit_bytes=VMEM_LIMIT),
            name='recurrent_layers',
        )(tok, x_in, jnp.transpose(conv_state, (0, 2, 1, 3)), lru_state, scales, rec_wx, rec_bx, rec_wy, rec_by, conv_w, conv_b, gate_wa, gate_ba, gate_wi, gate_bi, a_param, rec_wout, rec_bout, mlp_w1, mlp_b1, mlp_w2, mlp_b2, mlp_wd, mlp_bd)
        cache = (ROWS * WINDOW, 128)
        table = pltpu.VMEM((ROWS, 128), F32)
        part, k_out, v_out, slot_out = pl.pallas_call(
            attention_kernel,
            out_shape=[shape((N_CHUNK, 2, HALF, CHUNK), BF), shape(cache, BF), shape(cache, BF), shape((ROWS, WINDOW), jnp.int32)],
            in_specs=[pl.BlockSpec(memory_space=pltpu.SMEM)] + [ANY] * 12, out_specs=[ANY] * 4,
            scratch_shapes=body_scratch(N_SLOTS_B, 4) + [
                table, pltpu.VMEM((6, D), BF), pltpu.VMEM((1, ROWS), jnp.int32), table, table, pltpu.VMEM((ROWS, WINDOW), jnp.int32), pltpu.VMEM((ROWS, WINDOW), F32),
                pltpu.VMEM((ROWS, 128), jnp.int32), pltpu.VMEM((ROWS * HEADS, 128), F32), pltpu.VMEM((ROWS * HEADS, 128), F32), table, table,
                pltpu.VMEM((ROWS, 1024), BF), pltpu.VMEM((N_CHUNK, 2, HALF, CHUNK), BF), pltpu.SemaphoreType.DMA((6,)), pltpu.SemaphoreType.DMA((N_SLOTS_B, 2)), pltpu.SemaphoreType.DMA],
            compiler_params=pltpu.CompilerParams(vmem_limit_bytes=VMEM_LIMIT),
            name='attention_layer',
        )(tok_pos, tok, x_mid, scales, cosine, sine, k_cache.reshape(cache), v_cache.reshape(cache), slot_pos, attn_wq, attn_wk, attn_wv, attn_wo)
        x_out = pl.pallas_call(
            final_kernel,
            out_shape=shape((ROWS, D), BF),
            in_specs=[ANY] * 10, out_specs=ANY,
            scratch_shapes=body_scratch(N_SLOTS_C, 1) + [pltpu.VMEM((ROWS, 3072), BF), pltpu.VMEM((ROWS, 128), F32)] + COMM_SCRATCH + [
                pltpu.VMEM((6, D), BF), pltpu.VMEM((1, D), BF), pltpu.VMEM((3, 3072), BF), pltpu.VMEM((3, 3072), BF), pltpu.VMEM((3, D), BF), pltpu.SemaphoreType.DMA((7,))],
            compiler_params=pltpu.CompilerParams(collective_id=1, has_side_effects=True, vmem_limit_bytes=VMEM_LIMIT),
            name='last_mlp',
        )(x_mid, part, scales, attn_bo.reshape(1, D), mlp_w1, mlp_b1, mlp_w2, mlp_b2, mlp_wd, mlp_bd)
        return (x_out, jnp.transpose(conv_out, (0, 2, 1, 3)), lru_out, k_out.reshape(k_cache.shape), v_out.reshape(v_cache.shape), slot_out)

    return jax.shard_map(local_step, mesh=mesh, in_specs=in_specs, out_specs=out_specs, check_vma=False)
```

```python
import jax
import jax.numpy as jnp
import numpy as np
from jax import lax
from jax.experimental import pallas as pl
from jax.experimental.pallas import tpu as pltpu
from jax.sharding import PartitionSpec as P

ROPE_BASE = 10000.0
NORM_EPS = 1e-6
BF = jnp.bfloat16
F32 = jnp.float32
ROWS = 128
D = 4096
TILE = 256
CHUNK = 512
N_CHUNK = D // CHUNK
HALF = ROWS // 2
VMEM_LIMIT = 67043328


class Stream:
    def __init__(self, slots, sems, n_slots):
        self.slots, self.sems, self.n_slots = slots, sems, n_slots
        self.phases = []
        self.total = 0

    def add(self, n, *kinds):
        start = self.total
        self.phases.append((start, n, kinds))
        self.total += n
        return start, kinds

    def slot_of(self, t):
        return lax.rem(t, self.n_slots)

    def copies(self, kind, j, slot):
        return [pltpu.make_async_copy(src, self.slots.at[(slot,) + dst], self.sems.at[slot, i]) for i, (src, dst) in enumerate(kind(j))]

    def start_tile(self, kinds, j, slot):
        n = len(kinds)
        if n == 1:
            for c in self.copies(kinds[0], j, slot):
                c.start()
            return
        for which, kind in enumerate(kinds):
            @pl.when(lax.rem(j, n) == which)
            def _(kind=kind):
                for c in self.copies(kind, lax.div(j, n), slot):
                    c.start()

    def issue(self, t, lo, hi):
        for start, n, kinds in self.phases:
            if start + n <= lo or hi <= start:
                continue

            def go(start=start, kinds=kinds):
                self.start_tile(kinds, t - start, self.slot_of(t))

            if start <= lo and hi <= start + n:
                go()
            else:
                pl.when(jnp.logical_and(t >= start, t < start + n))(go)

    def prime(self):
        first = min(self.n_slots, self.total)
        for start, n, kinds in self.phases:
            stop = min(start + n, first)
            if start < stop:
                @pl.loop(start, stop)
                def _(t, start=start, kinds=kinds):
                    self.start_tile(kinds, t - start, self.slot_of(t))

    def wait(self, phase, j):
        start, kinds = phase
        slot = self.slot_of(start + j)
        for c in self.copies(kinds[0], lax.div(j, len(kinds)), slot):
            c.wait()
        return slot


def full(slot_rows):
    return (pl.ds(0, slot_rows), pl.ds(0, TILE))


def columns(ref, layer, rows):
    return lambda j: [(ref.at[layer, :, pl.ds(pl.multiple_of(j * TILE, TILE), TILE)], full(rows))]


def gelu(v):
    return jax.nn.gelu(v, approximate=True)


def f32(v):
    return v.astype(F32)


def cols(k, width=CHUNK):
    return pl.ds(pl.multiple_of(k * width, width), width)


class Comm:
    def __init__(self, part, r1, cs, r2, fin, r3, s1, q1, s2, q2, s3, q3):
        self.part, self.r1, self.cs, self.r2, self.fin, self.r3 = part, r1, cs, r2, fin, r3
        self.s1, self.q1, self.s2, self.q2, self.s3, self.q3 = s1, q1, s2, q2, s3, q3
        me = lax.axis_index('tp')
        self.mine = lax.rem(me, 2)
        self.other = 1 - self.mine
        self.partner = me + 1 - 2 * self.mine
        self.peer = lax.rem(me + 2, 4)

    def greet(self):
        for dev in (self.partner, self.peer):
            pl.semaphore_signal(pltpu.get_barrier_semaphore(), inc=1, device_id={'tp': dev}, device_id_type=pl.DeviceIdType.MESH)

    def meet(self):
        pl.semaphore_wait(pltpu.get_barrier_semaphore(), 2)

    def copy1(self, par, k):
        return pltpu.make_async_remote_copy(src_ref=self.part.at[k, self.other], dst_ref=self.r1.at[k], send_sem=self.s1.at[par, k], recv_sem=self.q1.at[par, k], device_id={'tp': self.partner}, device_id_type=pl.DeviceIdType.MESH)

    def copy2(self, par, k):
        return pltpu.make_async_remote_copy(src_ref=self.cs.at[k], dst_ref=self.r2.at[par, k], send_sem=self.s2.at[par, k], recv_sem=self.q2.at[par, k], device_id={'tp': self.peer}, device_id_type=pl.DeviceIdType.MESH)

    def copy3(self, par, k):
        return pltpu.make_async_remote_copy(src_ref=self.fin.at[k], dst_ref=self.r3.at[k], send_sem=self.s3.at[par, k], recv_sem=self.q3.at[par, k], device_id={'tp': self.partner}, device_id_type=pl.DeviceIdType.MESH)

    def chip_sum(self, par, k):
        self.copy1(par, k).wait_recv()
        self.cs[k] = (f32(self.part[k, self.mine]) + f32(self.r1[k])).astype(BF)
        self.copy2(par, k).start()

    def finish(self, par, update):
        @pl.loop(0, N_CHUNK)
        def _(k):
            self.copy2(par, k).wait_recv()
            total = (f32(self.cs[k]) + f32(self.r2[par, k])).astype(BF)
            self.fin[k] = total
            self.copy3(par, k).start()
            update(self.mine, k, f32(total))

            @pl.when(k >= 1)
            def _():
                self.copy3(par, k - 1).wait_recv()
                update(self.other, k - 1, f32(self.r3[k - 1]))

        self.copy3(par, N_CHUNK - 1).wait_recv()
        update(self.other, N_CHUNK - 1, f32(self.r3[N_CHUNK - 1]))

        @pl.loop(0, N_CHUNK)
        def _(k):
            self.copy1(par, k).wait_send()
            self.copy2(par, k).wait_send()
            self.copy3(par, k).wait_send()


def fold_lanes(v):
    acc = v[:, 0:128]
    for i in range(1, v.shape[1] // 128):
        acc = acc + v[:, 128 * i:128 * (i + 1)]
    return acc


class Body:
    def __init__(self, stream, comm, x, n, hid, ss, nscale):
        self.stream, self.comm, self.x, self.n, self.hid, self.ss, self.nscale = stream, comm, x, n, hid, ss, nscale
        self.n_ar = 0

    def squares(self):
        self.ss[...] = jnp.zeros_like(self.ss)

        @pl.loop(0, N_CHUNK)
        def _(k):
            v = f32(self.x[:, cols(k)])
            self.ss[...] += fold_lanes(v * v)

    def norm(self, row):
        scale = lax.rsqrt(jnp.sum(self.ss[...], axis=-1, keepdims=True) * (1.0 / D) + NORM_EPS)

        @pl.loop(0, N_CHUNK)
        def _(k):
            gain = 1.0 + f32(self.nscale[row // 2, row % 2:row % 2 + 1, cols(k)])
            self.n[:, cols(k)] = (f32(self.x[:, cols(k)]) * scale * gain).astype(BF)

    def updater(self, bias, row):
        def update(half, k, u):
            rows = pl.ds(pl.multiple_of(half * HALF, HALF), HALF)
            new = (f32(self.x[rows, cols(k)]) + u + f32(bias[cols(k)].reshape(1, CHUNK) if row is None else bias[row:row + 1, cols(k)])).astype(BF)
            self.x[rows, cols(k)] = new
            v = f32(new)
            self.ss[rows, :] += fold_lanes(v * v)

        return update

    def all_reduce(self, bias, row):
        par = self.n_ar % 2
        self.n_ar += 1
        self.ss[...] = jnp.zeros_like(self.ss)
        self.comm.finish(par, self.updater(bias, row))

    def down(self, phase, depth, per_chunk, lhs):
        st, comm, par = self.stream, self.comm, self.n_ar % 2
        start = phase[0]
        ahead = start + st.n_slots
        stop = ahead + per_chunk * N_CHUNK

        @pl.loop(0, N_CHUNK)
        def _(k):
            for h in range(2):
                if per_chunk == 2 or h == 0:
                    slot = st.wait(phase, k * per_chunk + h)
                off = 0 if per_chunk == 2 else h * depth
                prod = jnp.dot(lhs[...], st.slots[slot, off:off + depth, :], preferred_element_type=F32).astype(BF)
                for r in range(2):
                    comm.part[k, r, :, h * TILE:(h + 1) * TILE] = prod[r * HALF:(r + 1) * HALF]
            for h in range(per_chunk):
                st.issue(ahead + k * per_chunk + h, ahead, stop)
            comm.copy1(par, k).start()

            @pl.when(k >= 1)
            def _():
                comm.chip_sum(par, k - 1)

        comm.chip_sum(par, N_CHUNK - 1)

    def mlp(self, up, down, layer, b1, b2, bd):
        st = self.stream
        start = up[0]
        ahead = start + st.n_slots
        stop = ahead + 24

        @pl.loop(0, 12)
        def _(i):
            s0 = st.wait(up, 2 * i)
            s1 = st.wait(up, 2 * i + 1)
            g = jnp.dot(self.n[...], st.slots[s0], preferred_element_type=F32)
            v = jnp.dot(self.n[...], st.slots[s1], preferred_element_type=F32)
            st.issue(ahead + 2 * i, ahead, stop)
            st.issue(ahead + 2 * i + 1, ahead, stop)
            g = g + f32(b1[layer:layer + 1, cols(i, TILE)])
            v = v + f32(b2[layer:layer + 1, cols(i, TILE)])
            self.hid[:, cols(i, TILE)] = (gelu(g) * v).astype(BF)

        self.down(down, 3072, 2, self.hid)
        self.all_reduce(bd, layer)


    def recurrent(self, x_tiles, mixed, y_tiles, out_tiles, layer, v, outs):
        st = self.stream
        ahead = x_tiles[0] + st.n_slots
        stop = ahead + 11

        def dots(phase, tiles):
            slots = [st.wait(phase, i) for i in tiles]
            return [jnp.dot(self.n[...], st.slots[slot], preferred_element_type=F32) for slot in slots]

        def put_x(i, g):
            v.xb[layer, :, cols(i, TILE)] = (g + f32(v.bx[layer:layer + 1, cols(i, TILE)])).astype(BF)

        @pl.loop(0, 2)
        def _(p):
            for h, g in enumerate(dots(x_tiles, [2 * p, 2 * p + 1])):
                put_x(2 * p + h, g)
            for h in range(2):
                st.issue(ahead + 2 * p + h, ahead, stop)

        if layer == 0:
            self.comm.meet()
        last_x, = dots(x_tiles, [4])
        g, = dots(mixed, [0])
        for h in range(2):
            st.issue(ahead + 4 + h, ahead, stop)
        put_x(4, last_x)
        v.xb[layer, :, 1280:1408] = (g[:, 0:128] + f32(v.bx[layer:layer + 1, 1280:1408])).astype(BF)
        v.yg[...] = gelu(g[:, 128:256] + f32(v.by[layer:layer + 1, 1280:1408]))

        outs.wait_inputs(layer)
        pos = v.tokc[...]

        @pl.loop(0, 11)
        def _(i):
            c = cols(i, 128)
            acc = f32(v.cb[layer:layer + 1, c]) + f32(v.cw[layer, 0:1, c]) * f32(v.xb[layer, :, c])
            for j in range(3):
                acc = acc + jnp.where(pos >= 3 - j, f32(v.conv[layer, j, :, c]), 0.0) * f32(v.cw[layer, 3 - j:4 - j, c])
            v.xc[:, c] = acc.astype(BF)

        for b in range(8):
            c = slice(176 * b, 176 * (b + 1))
            xc = v.xc[:, c]
            v.rp[:, c] = jnp.dot(xc, v.ga[layer, b], preferred_element_type=F32)
            v.ip[:, c] = jnp.dot(xc, v.gi[layer, b], preferred_element_type=F32)

        def gate(c, reset):
            rate = -8.0 * jax.nn.softplus(v.ap[layer:layer + 1, c])
            decay = jnp.exp(rate * jax.nn.sigmoid(v.rp[:, c] + f32(v.gba[layer:layer + 1, c])))
            into = jnp.sqrt(1.0 - decay * decay)
            decay = jnp.where(reset, 0.0, decay)
            into = jnp.where(reset, 1.0, into)
            new = decay * v.lru[layer, :, c] + into * jax.nn.sigmoid(v.ip[:, c] + f32(v.gbi[layer:layer + 1, c])) * f32(v.xc[:, c])
            v.lru[layer, :, c] = new
            return new

        def put_y(i, g):
            for h in range(2):
                c = cols(2 * i + h, 128)
                new = gate(c, pos == 0)
                y = gelu(g[:, 128 * h:128 * (h + 1)] + f32(v.by[layer:layer + 1, c]))
                v.gated[:, c] = (new * y).astype(BF)

        @pl.loop(0, 2)
        def _(p):
            for h, g in enumerate(dots(y_tiles, [2 * p, 2 * p + 1])):
                put_y(2 * p + h, g)
            for h in range(2):
                st.issue(ahead + 6 + 2 * p + h, ahead, stop)

        g, = dots(y_tiles, [4])
        st.issue(ahead + 10, ahead, stop)
        put_y(4, g)
        c = slice(1280, 1408)
        v.gated[:, c] = (gate(c, pos == 0) * v.yg[...]).astype(BF)
        outs.write(layer)
        self.down(out_tiles, 1408, 1, v.gated)
        self.all_reduce(v.bout, layer)
        outs.wait_write(layer)


def add_mlp(stream, w1, w2, wd, layer):
    up = stream.add(24, columns(w1, layer, D), columns(w2, layer, D))
    return up, stream.add(16, columns(wd, layer, 3072))


class Names:
    def __init__(self, **kw):
        self.__dict__.update(kw)


class StateCopies:
    def __init__(self, ins, xb_out, lru_out, v, in_sem, out_sem):
        self.ins, self.xb_out, self.lru_out, self.v, self.in_sem, self.out_sem = ins, xb_out, lru_out, v, in_sem, out_sem

    def inputs(self, layer):
        return [pltpu.make_async_copy(src.at[layer], dst.at[layer], self.in_sem.at[layer, i]) for i, (src, dst) in enumerate(self.ins)]

    def start_inputs(self, layer):
        for c in self.inputs(layer):
            c.start()

    def wait_inputs(self, layer):
        for c in self.inputs(layer):
            c.wait()

    def outputs(self, layer):
        pairs = [(self.v.xb.at[layer], self.xb_out.at[layer]), (self.v.lru.at[layer], self.lru_out.at[layer])]
        return [pltpu.make_async_copy(src, dst, self.out_sem.at[layer, i]) for i, (src, dst) in enumerate(pairs)]

    def write(self, layer):
        for c in self.outputs(layer):
            c.start()

    def wait_write(self, layer):
        for c in self.outputs(layer):
            c.wait()


N_SLOTS_A = 20
N_SLOTS_B = 22
N_SLOTS_C = 24

COMM_SCRATCH = [
    pltpu.VMEM((N_CHUNK, 2, HALF, CHUNK), BF), pltpu.VMEM((N_CHUNK, HALF, CHUNK), BF), pltpu.VMEM((N_CHUNK, HALF, CHUNK), BF),
    pltpu.VMEM((2, N_CHUNK, HALF, CHUNK), BF), pltpu.VMEM((N_CHUNK, HALF, CHUNK), BF), pltpu.VMEM((N_CHUNK, HALF, CHUNK), BF),
] + [pltpu.SemaphoreType.DMA((2, N_CHUNK)) for _ in range(6)]


def body_scratch(n_slots, n_pieces):
    return [pltpu.VMEM((n_slots, D, TILE), BF), pltpu.SemaphoreType.DMA((n_slots, n_pieces)), pltpu.VMEM((ROWS, D), BF), pltpu.VMEM((ROWS, D), BF)]


def recurrent_kernel(tok, x_in, conv, lru, nscale, wx, bx, wy, by, cw, cb, ga, gba, gi, gbi, ap, wout, bout, w1, b1, w2, b2, wd, bd, *refs):
    x_out, xb_out, lru_out = refs[:3]
    slots, sems, x, n, hid, ss = refs[3:9]
    comm = Comm(*refs[9:21])
    small = refs[21:35]
    v_tok, v_ns, v_bx, v_by, v_cw, v_cb, v_gba, v_gbi, v_ap, v_bout, v_b1, v_b2, v_bd, small_sem = small
    v_conv, v_lru, v_ga, v_gi, xb, yg, xc, rp, ip, gated, tokc, in_sem, out_sem = refs[35:]
    stream = Stream(slots, sems, N_SLOTS_A)
    v = Names(bx=v_bx, by=v_by, cw=v_cw, cb=v_cb, ga=v_ga, gba=v_gba, gi=v_gi, gbi=v_gbi, ap=v_ap, bout=v_bout, conv=v_conv, lru=v_lru, xb=xb, yg=yg, xc=xc, rp=rp, ip=ip, gated=gated, tokc=tokc)
    outs = StateCopies([(conv, v_conv), (lru, v_lru), (ga, v_ga), (gi, v_gi)], xb_out, lru_out, v, in_sem, out_sem)
    body = Body(stream, comm, x, n, hid, ss, v_ns)

    plan = []
    for layer in range(2):
        xt = stream.add(5, columns(wx, layer, D))
        mixed = stream.add(1, lambda j, layer=layer: [(wx.at[layer, :, 1280:1408], (pl.ds(0, D), pl.ds(0, 128))), (wy.at[layer, :, 1280:1408], (pl.ds(0, D), pl.ds(128, 128)))])
        yt = stream.add(5, columns(wy, layer, D))
        ot = stream.add(8, lambda j, layer=layer: [(wout.at[layer, :, pl.ds(pl.multiple_of(j * CHUNK + h * TILE, TILE), TILE)], (pl.ds(h * 1408, 1408), pl.ds(0, TILE))) for h in range(2)])
        up, down = add_mlp(stream, w1, w2, wd, layer)
        plan.append((xt, mixed, yt, ot, up, down))

    pairs = [(x_in, x), (tok, v_tok), (nscale, v_ns), (bx, v_bx), (by, v_by), (cw, v_cw), (cb, v_cb), (gba, v_gba), (gbi, v_gbi), (ap, v_ap), (bout, v_bout), (b1, v_b1), (b2, v_b2), (bd, v_bd)]
    early = [pltpu.make_async_copy(s, d, small_sem.at[i]) for i, (s, d) in enumerate(pairs)]
    for c in early:
        c.start()
    comm.greet()
    stream.prime()
    outs.start_inputs(0)
    outs.start_inputs(1)
    for c in early:
        c.wait()
    tokc[...] = jnp.broadcast_to(v_tok[...], (ROWS, 128)).T
    body.squares()
    for layer in range(2):
        xt, mixed, yt, ot, up, down = plan[layer]
        body.norm(2 * layer)
        body.recurrent(xt, mixed, yt, ot, layer, v, outs)
        body.norm(2 * layer + 1)
        body.mlp(up, down, layer, v_b1, v_b2, v_bd)
    last = pltpu.make_async_copy(x, x_out, small_sem.at[0])
    last.start()
    last.wait()


def final_kernel(x_in, part_in, nscale, bo, w1, b1, w2, b2, wd, bd, *refs):
    x, slots, sems, n, hid, ss = refs[:6]
    comm = Comm(*refs[6:18])
    v_ns, v_bo, v_b1, v_b2, v_bd, small_sem = refs[18:]
    stream = Stream(slots, sems, N_SLOTS_C)
    body = Body(stream, comm, x, n, hid, ss, v_ns)
    up, down = add_mlp(stream, w1, w2, wd, 2)
    pairs = [(part_in, comm.part), (x_in, x), (nscale, v_ns), (bo, v_bo), (b1, v_b1), (b2, v_b2), (bd, v_bd)]
    early = [pltpu.make_async_copy(s, d, small_sem.at[i]) for i, (s, d) in enumerate(pairs)]
    for c in early:
        c.start()
    comm.greet()
    stream.prime()
    early[0].wait()
    comm.meet()

    @pl.loop(0, N_CHUNK)
    def _(k):
        comm.copy1(0, k).start()

    for c in early[1:]:
        c.wait()

    @pl.loop(0, N_CHUNK)
    def _(k):
        comm.chip_sum(0, k)

    body.all_reduce(v_bo, None)
    body.norm(5)
    body.mlp(up, down, 2, v_b1, v_b2, v_bd)


GROUP = 4
N_GROUP = ROWS // GROUP
WINDOW = 1024
HEADS = 8
LAG = 4
FREQ = np.zeros((1, 128), np.float32)
FREQ[0, :32] = FREQ[0, 32:64] = np.float32(ROPE_BASE) ** (-np.arange(32, dtype=np.float32) / 32)


def attention_kernel(pos_s, tok, x_in, nscale, freq, conv, xb, lru, k_cache, v_cache, slot_pos, wq, wk, wv, wo, part_out, conv_out, lru_out, k_out, v_out, slot_out,
                     slots, sems, x, n, ss, v_ns, v_tok, v_freq, v_cos, v_sin, v_conv, v_lru, v_slot, bias, tokc, q3, o3, k_new, v_new, o_bf, part, small_sem, state_sem, out_sem):
    stream = Stream(slots, sems, N_SLOTS_B)
    body = Body(stream, None, x, n, None, ss, v_ns)
    qt = stream.add(4, lambda j: [(wq.at[:, cols(j, TILE)], full(D))])
    kvt = stream.add(1, lambda j: [(wk, (pl.ds(0, D), pl.ds(0, 128))), (wv, (pl.ds(0, D), pl.ds(128, 128)))])

    def group_rows(j):
        return pl.ds(pl.multiple_of(j * GROUP * WINDOW, GROUP * WINDOW), GROUP * WINDOW)

    ct = stream.add(N_GROUP, lambda j: [(src.at[group_rows(j)], (pl.ds(0, D), pl.ds(128 * i, 128))) for i, src in enumerate((k_cache, v_cache))])
    ot = stream.add(4, lambda j: [(wo.at[:, cols(4 * j + h, TILE)], (pl.ds(1024 * h, 1024), pl.ds(0, TILE))) for h in range(4)])

    def copies(pairs, sem):
        return [pltpu.make_async_copy(a, b, sem.at[i]) for i, (a, b) in enumerate(pairs)]

    def start(group):
        for c in group:
            c.start()

    def finish(group):
        for c in group:
            c.wait()

    early = copies([(x_in, x), (tok, v_tok), (nscale, v_ns), (freq, v_freq), (slot_pos, v_slot)], small_sem)
    start(early)
    stream.prime()
    states = copies([(conv.at[:, 1:3], v_conv.at[:, 0:2]), (xb, v_conv.at[:, 2]), (lru, v_lru)], state_sem)
    start(states)
    finish(early)
    tokc[...] = jnp.broadcast_to(v_tok[...], (ROWS, 128)).T
    body.squares()
    body.norm(4)

    pos = tokc[...]
    target = lax.rem(pos, WINDOW)
    lane = lax.broadcasted_iota(jnp.int32, (ROWS, 128), 1)
    angle = f32(pos) * v_freq[...]
    v_cos[...] = jnp.cos(angle)
    v_sin[...] = jnp.sin(angle) * jnp.where(lane < 32, -1.0, 1.0)

    @pl.loop(0, WINDOW // 128)
    def _(i):
        now = jnp.where(lane + i * 128 == target, pos, v_slot[:, cols(i, 128)])
        v_slot[:, cols(i, 128)] = now
        age = pos - now
        good = (now >= 0) & (age >= 0) & (age < WINDOW)
        bias[:, cols(i, 128)] = jnp.where(good, 0.0, -jnp.inf)

    def rope(val):
        other = jnp.where(lane < 32, pltpu.roll(val, 96, 1), pltpu.roll(val, 32, 1))
        return val * v_cos[...] + other * v_sin[...]

    ahead = stream.n_slots

    @pl.loop(0, 2)
    def _(p):
        got = [stream.wait(qt, 2 * p + i) for i in range(2)]
        for i, slot in enumerate(got):
            g = jnp.dot(n[...], slots[slot], preferred_element_type=F32)
            for h in range(2):
                q3[pl.ds(4 * p + 2 * i + h, ROWS, stride=HEADS), :] = f32(rope(g[:, 128 * h:128 * (h + 1)]).astype(BF))
        for i in range(2):
            stream.issue(ahead + 2 * p + i, ahead, ahead + 4)

    slot = stream.wait(kvt, 0)
    g = jnp.dot(n[...], slots[slot], preferred_element_type=F32)
    stream.issue(ahead + 4, ahead + 4, ahead + 5)
    k_new[...] = f32(rope(g[:, 0:128]).astype(BF))
    v_new[...] = f32(g[:, 128:256].astype(BF))

    finish(states)
    results = copies([(v_conv, conv_out), (v_lru, lru_out), (v_slot, slot_out)], state_sem)
    start(results)

    def outputs(j):
        slot = stream.slot_of(ct[0] + j)
        return [pltpu.make_async_copy(slots.at[slot, :, pl.ds(128 * i, 128)], dst.at[group_rows(j)], out_sem.at[slot, i]) for i, dst in enumerate((k_out, v_out))]

    row16 = lax.broadcasted_iota(jnp.int32, (16, 128), 0)
    ahead = ct[0] - LAG + stream.n_slots
    nt = (((1,), (1,)), ((), ()))

    @pl.loop(0, N_GROUP // 2)
    def _(p):
        got = [stream.wait(ct, 2 * p + g) for g in range(2)]
        for g, slot in enumerate(got):
            for r in range(GROUP):
                seq = (2 * p + g) * GROUP + r
                spot = lax.rem(pos_s[seq], WINDOW)
                base = pl.multiple_of(r * WINDOW + lax.div(spot, 16) * 16, 16)
                for i, new in enumerate((k_new, v_new)):
                    here = (slot, pl.ds(base, 16), pl.ds(128 * i, 128))
                    slots[here] = jnp.where(row16 == lax.rem(spot, 16), new[pl.ds(seq, 1), :], f32(slots[here])).astype(BF)
            start(outputs(2 * p + g))

        pairs = [(slot, h) for slot in got for h in range(GROUP // 2)]
        first = 2 * p * GROUP
        scores = []
        for i, (slot, h) in enumerate(pairs):
            q = q3[pl.ds(pl.multiple_of((first + 2 * i) * HEADS, 2 * HEADS), 2 * HEADS), :].astype(BF)
            halves = []
            for e in range(2):
                r = 2 * h + e
                keys = slots[slot, r * WINDOW:(r + 1) * WINDOW, 0:128]
                score = lax.dot_general(q, keys, nt, preferred_element_type=F32)[HEADS * e:HEADS * (e + 1)] * (128 ** -0.5)
                halves.append(score + bias[pl.ds(first + 2 * i + e, 1), :])
            scores.append(jnp.concatenate(halves, axis=0))
        probs = []
        for score in scores:
            e = jnp.exp(score - jnp.max(score, axis=-1, keepdims=True))
            probs.append((e / jnp.sum(e, axis=-1, keepdims=True)).astype(BF))
        for i, (slot, h) in enumerate(pairs):
            halves = []
            for e in range(2):
                r = 2 * h + e
                values = slots[slot, r * WINDOW:(r + 1) * WINDOW, 128:256]
                halves.append(jnp.dot(probs[i], values, preferred_element_type=F32)[HEADS * e:HEADS * (e + 1)])
            o3[pl.ds(pl.multiple_of((first + 2 * i) * HEADS, 2 * HEADS), 2 * HEADS), :] = jnp.concatenate(halves, axis=0)

        @pl.when(2 * p >= LAG)
        def _():
            for g in range(2):
                finish(outputs(2 * p + g - LAG))
                stream.issue(ahead + 2 * p + g, ahead + LAG, ahead + N_GROUP)

    for h in range(HEADS):
        o_bf[:, 128 * h:128 * (h + 1)] = o3[pl.ds(h, ROWS, stride=HEADS), :].astype(BF)

    @pl.loop(0, 4)
    def _(j):
        slot = stream.wait(ot, j)
        for h in range(4):
            prod = jnp.dot(o_bf[...], slots[slot, 1024 * h:1024 * (h + 1), :], preferred_element_type=F32).astype(BF)
            for r in range(2):
                part[2 * j + h // 2, r, :, (h % 2) * TILE:(h % 2 + 1) * TILE] = prod[r * HALF:(r + 1) * HALF]

    last = pltpu.make_async_copy(part, part_out, small_sem.at[0])
    last.start()
    for j in range(N_GROUP - LAG, N_GROUP):
        finish(outputs(j))
    finish(results)
    last.wait()


ANY = pl.BlockSpec(memory_space=pl.ANY)


def io_specs():
    in_specs = (P('dp', None), P('dp'), P(None, 'dp', None, 'tp'), P(None, 'dp', 'tp'), P('dp', None, None), P('dp', None, None), P('dp', None),
                P(), P(None, None, 'tp'), P(None, 'tp'), P(None, None, 'tp'), P(None, 'tp'), P(None, None, 'tp'), P(None, 'tp'),
                P(None, 'tp', None, None), P(None, 'tp'), P(None, 'tp', None, None), P(None, 'tp'), P(None, 'tp'), P(None, 'tp', None), P(),
                P(None, 'tp'), P(), P(), P('tp', None), P(),
                P(None, None, 'tp'), P(None, 'tp'), P(None, None, 'tp'), P(None, 'tp'), P(None, 'tp', None), P())
    out_specs = (P('dp', None), P(None, 'dp', None, 'tp'), P(None, 'dp', 'tp'), P('dp', None, None), P('dp', None, None), P('dp', None))
    return in_specs, out_specs


def solution(mesh):
    in_specs, out_specs = io_specs()
    shape = jax.ShapeDtypeStruct

    def local_step(x_in, tok_pos, conv_state, lru_state, k_cache, v_cache, slot_pos, norm_scale, rec_wx, rec_bx, rec_wy, rec_by, conv_w, conv_b, gate_wa, gate_ba, gate_wi, gate_bi, a_param, rec_wout, rec_bout, attn_wq, attn_wk, attn_wv, attn_wo, attn_bo, mlp_w1, mlp_b1, mlp_w2, mlp_b2, mlp_wd, mlp_bd):
        tok = tok_pos.reshape(1, ROWS)
        conv_t = jnp.transpose(conv_state, (0, 2, 1, 3))
        vec = pltpu.VMEM((2, 1408), BF)
        x_mid, xb, lru_mid = pl.pallas_call(
            recurrent_kernel,
            out_shape=[shape((ROWS, D), BF), shape((2, ROWS, 1408), BF), shape((2, ROWS, 1408), F32)],
            in_specs=[ANY] * 24, out_specs=[ANY] * 3,
            scratch_shapes=body_scratch(N_SLOTS_A, 2) + [pltpu.VMEM((ROWS, 3072), BF), pltpu.VMEM((ROWS, 128), F32)] + COMM_SCRATCH + [
                pltpu.VMEM((1, ROWS), jnp.int32), pltpu.VMEM((3, 2, D), BF), vec, vec, pltpu.VMEM((2, 4, 1408), BF), vec, vec, vec, pltpu.VMEM((2, 1408), F32),
                pltpu.VMEM((2, D), BF), pltpu.VMEM((3, 3072), BF), pltpu.VMEM((3, 3072), BF), pltpu.VMEM((3, D), BF), pltpu.SemaphoreType.DMA((14,)),
                pltpu.VMEM((2, 3, ROWS, 1408), BF), pltpu.VMEM((2, ROWS, 1408), F32), pltpu.VMEM((2, 8, 176, 176), BF), pltpu.VMEM((2, 8, 176, 176), BF),
                pltpu.VMEM((2, ROWS, 1408), BF), pltpu.VMEM((ROWS, 128), F32), pltpu.VMEM((ROWS, 1408), BF), pltpu.VMEM((ROWS, 1408), F32), pltpu.VMEM((ROWS, 1408), F32),
                pltpu.VMEM((ROWS, 1408), BF), pltpu.VMEM((ROWS, 128), jnp.int32), pltpu.SemaphoreType.DMA((2, 4)), pltpu.SemaphoreType.DMA((2, 3))],
            compiler_params=pltpu.CompilerParams(collective_id=0, has_side_effects=True, vmem_limit_bytes=VMEM_LIMIT),
            name='recurrent_layers',
        )(tok, x_in, conv_t, lru_state, norm_scale, rec_wx, rec_bx, rec_wy, rec_by, conv_w, conv_b, gate_wa, gate_ba, gate_wi, gate_bi, a_param, rec_wout, rec_bout, mlp_w1, mlp_b1, mlp_w2, mlp_b2, mlp_wd, mlp_bd)
        cache = (ROWS * WINDOW, 128)
        table = pltpu.VMEM((ROWS, 128), F32)
        part, conv_out, lru_out, k_out, v_out, slot_out = pl.pallas_call(
            attention_kernel,
            out_shape=[shape((N_CHUNK, 2, HALF, CHUNK), BF), shape((2, 3, ROWS, 1408), BF), shape((2, ROWS, 1408), F32), shape(cache, BF), shape(cache, BF), shape((ROWS, WINDOW), jnp.int32)],
            in_specs=[pl.BlockSpec(memory_space=pltpu.SMEM)] + [ANY] * 14, out_specs=[ANY] * 6,
            scratch_shapes=body_scratch(N_SLOTS_B, 4) + [
                table, pltpu.VMEM((3, 2, D), BF), pltpu.VMEM((1, ROWS), jnp.int32), pltpu.VMEM((1, 128), F32), table, table, pltpu.VMEM((2, 3, ROWS, 1408), BF), pltpu.VMEM((2, ROWS, 1408), F32), pltpu.VMEM((ROWS, WINDOW), jnp.int32), pltpu.VMEM((ROWS, WINDOW), F32),
                pltpu.VMEM((ROWS, 128), jnp.int32), pltpu.VMEM((ROWS * HEADS, 128), F32), pltpu.VMEM((ROWS * HEADS, 128), F32), table, table,
                pltpu.VMEM((ROWS, 1024), BF), pltpu.VMEM((N_CHUNK, 2, HALF, CHUNK), BF), pltpu.SemaphoreType.DMA((5,)), pltpu.SemaphoreType.DMA((3,)), pltpu.SemaphoreType.DMA((N_SLOTS_B, 2))],
            compiler_params=pltpu.CompilerParams(vmem_limit_bytes=VMEM_LIMIT),
            name='attention_layer',
        )(tok_pos, tok, x_mid, norm_scale, jnp.asarray(FREQ), conv_t, xb, lru_mid, k_cache.reshape(cache), v_cache.reshape(cache), slot_pos, attn_wq, attn_wk, attn_wv, attn_wo)
        x_out = pl.pallas_call(
            final_kernel,
            out_shape=shape((ROWS, D), BF),
            in_specs=[ANY] * 10, out_specs=pl.BlockSpec(memory_space=pltpu.VMEM),
            scratch_shapes=body_scratch(N_SLOTS_C, 1)[:3] + [pltpu.VMEM((ROWS, 3072), BF), pltpu.VMEM((ROWS, 128), F32)] + COMM_SCRATCH + [
                pltpu.VMEM((3, 2, D), BF), pltpu.VMEM((D,), BF), pltpu.VMEM((3, 3072), BF), pltpu.VMEM((3, 3072), BF), pltpu.VMEM((3, D), BF), pltpu.SemaphoreType.DMA((7,))],
            compiler_params=pltpu.CompilerParams(collective_id=1, has_side_effects=True, vmem_limit_bytes=VMEM_LIMIT),
            name='last_mlp',
        )(x_mid, part, norm_scale, attn_bo, mlp_w1, mlp_b1, mlp_w2, mlp_b2, mlp_wd, mlp_bd)
        return (x_out, jnp.transpose(conv_out, (0, 2, 1, 3)), lru_out, k_out.reshape(k_cache.shape), v_out.reshape(v_cache.shape), slot_out)

    return jax.shard_map(local_step, mesh=mesh, in_specs=in_specs, out_specs=out_specs, check_vma=False)
```

```python
import jax
import jax.numpy as jnp
import numpy as np
from jax import lax
from jax.experimental import pallas as pl
from jax.experimental.pallas import tpu as pltpu
from jax.sharding import PartitionSpec as P

ROPE_BASE = 10000.0
NORM_EPS = 1e-6
BF = jnp.bfloat16
F32 = jnp.float32
ROWS = 128
LOCAL = 1408
D = 4096
TILE = 256
CHUNK = 512
N_CHUNK = D // CHUNK
HALF = ROWS // 2
VMEM_LIMIT = 67043328


class Stream:
    def __init__(self, slots, sems, n_slots):
        self.slots, self.sems, self.n_slots = slots, sems, n_slots
        self.phases = []
        self.total = 0

    def add(self, n, *kinds):
        start = self.total
        self.phases.append((start, n, kinds))
        self.total += n
        return start, kinds

    def slot_of(self, t):
        return lax.rem(t, self.n_slots)

    def copies(self, kind, j, slot):
        return [pltpu.make_async_copy(src, self.slots.at[(slot,) + dst], self.sems.at[slot, i]) for i, (src, dst) in enumerate(kind(j))]

    def start_tile(self, kinds, j, slot):
        n = len(kinds)
        if n == 1:
            for c in self.copies(kinds[0], j, slot):
                c.start()
            return
        for which, kind in enumerate(kinds):
            @pl.when(lax.rem(j, n) == which)
            def _(kind=kind):
                for c in self.copies(kind, lax.div(j, n), slot):
                    c.start()

    def issue(self, t, lo, hi):
        for start, n, kinds in self.phases:
            if start + n <= lo or hi <= start:
                continue

            def go(start=start, kinds=kinds):
                self.start_tile(kinds, t - start, self.slot_of(t))

            if start <= lo and hi <= start + n:
                go()
            else:
                pl.when(jnp.logical_and(t >= start, t < start + n))(go)

    def prime(self, lo, hi):
        for start, n, kinds in self.phases:
            first, stop = max(start, lo), min(start + n, hi, self.n_slots)
            if first < stop:
                @pl.loop(first, stop)
                def _(t, start=start, kinds=kinds):
                    self.start_tile(kinds, t - start, self.slot_of(t))

    def wait(self, phase, j):
        start, kinds = phase
        slot = self.slot_of(start + j)
        for c in self.copies(kinds[0], lax.div(j, len(kinds)), slot):
            c.wait()
        return slot


def full(slot_rows):
    return (pl.ds(0, slot_rows), pl.ds(0, TILE))


def columns(ref, layer, rows):
    return lambda j: [(ref.at[layer, :, pl.ds(pl.multiple_of(j * TILE, TILE), TILE)], full(rows))]


def gelu(v):
    return jax.nn.gelu(v, approximate=True)


def f32(v):
    return v.astype(F32)


def cols(k, width=CHUNK):
    return pl.ds(pl.multiple_of(k * width, width), width)


class Comm:
    def __init__(self, part, r1, cs, r2, fin, r3, s1, q1, s2, q2, s3, q3):
        self.part, self.r1, self.cs, self.r2, self.fin, self.r3 = part, r1, cs, r2, fin, r3
        self.s1, self.q1, self.s2, self.q2, self.s3, self.q3 = s1, q1, s2, q2, s3, q3
        me = lax.axis_index('tp')
        self.mine = lax.rem(me, 2)
        self.other = 1 - self.mine
        self.partner = me + 1 - 2 * self.mine
        self.peer = lax.rem(me + 2, 4)

    def greet(self):
        for dev in (self.partner, self.peer):
            pl.semaphore_signal(pltpu.get_barrier_semaphore(), inc=1, device_id={'tp': dev}, device_id_type=pl.DeviceIdType.MESH)

    def meet(self):
        pl.semaphore_wait(pltpu.get_barrier_semaphore(), 2)

    def copy1(self, par, k):
        return pltpu.make_async_remote_copy(src_ref=self.part.at[k, self.other], dst_ref=self.r1.at[k], send_sem=self.s1.at[par, k], recv_sem=self.q1.at[par, k], device_id={'tp': self.partner}, device_id_type=pl.DeviceIdType.MESH)

    def copy2(self, par, k):
        return pltpu.make_async_remote_copy(src_ref=self.cs.at[k], dst_ref=self.r2.at[par, k], send_sem=self.s2.at[par, k], recv_sem=self.q2.at[par, k], device_id={'tp': self.peer}, device_id_type=pl.DeviceIdType.MESH)

    def copy3(self, par, k):
        return pltpu.make_async_remote_copy(src_ref=self.fin.at[k], dst_ref=self.r3.at[k], send_sem=self.s3.at[par, k], recv_sem=self.q3.at[par, k], device_id={'tp': self.partner}, device_id_type=pl.DeviceIdType.MESH)

    def chip_sum(self, par, k):
        self.copy1(par, k).wait_recv()
        self.cs[k] = (f32(self.part[k, self.mine]) + f32(self.r1[k])).astype(BF)
        self.copy2(par, k).start()

    def finish(self, par, update):
        @pl.loop(0, N_CHUNK)
        def _(k):
            self.copy2(par, k).wait_recv()
            total = (f32(self.cs[k]) + f32(self.r2[par, k])).astype(BF)
            self.fin[k] = total
            self.copy3(par, k).start()
            update(self.mine, k, f32(total))

            @pl.when(k >= 1)
            def _():
                self.copy3(par, k - 1).wait_recv()
                update(self.other, k - 1, f32(self.r3[k - 1]))

        self.copy3(par, N_CHUNK - 1).wait_recv()
        update(self.other, N_CHUNK - 1, f32(self.r3[N_CHUNK - 1]))

        @pl.loop(0, N_CHUNK)
        def _(k):
            self.copy1(par, k).wait_send()
            self.copy2(par, k).wait_send()
            self.copy3(par, k).wait_send()


def fold_lanes(v):
    acc = v[:, 0:128]
    for i in range(1, v.shape[1] // 128):
        acc = acc + v[:, 128 * i:128 * (i + 1)]
    return acc


class Body:
    def __init__(self, stream, comm, x, n, hid, ss, nscale):
        self.stream, self.comm, self.x, self.n, self.hid, self.ss, self.nscale = stream, comm, x, n, hid, ss, nscale
        self.n_ar = 0

    def squares(self):
        self.ss[...] = jnp.zeros_like(self.ss)

        @pl.loop(0, N_CHUNK)
        def _(k):
            v = f32(self.x[:, cols(k)])
            self.ss[...] += fold_lanes(v * v)

    def norm(self, row):
        scale = lax.rsqrt(jnp.sum(self.ss[...], axis=-1, keepdims=True) * (1.0 / D) + NORM_EPS)

        @pl.loop(0, N_CHUNK)
        def _(k):
            gain = 1.0 + f32(self.nscale[row // 2, row % 2:row % 2 + 1, cols(k)])
            self.n[:, cols(k)] = (f32(self.x[:, cols(k)]) * scale * gain).astype(BF)

    def updater(self, bias, row):
        def update(half, k, u):
            rows = pl.ds(pl.multiple_of(half * HALF, HALF), HALF)
            new = (f32(self.x[rows, cols(k)]) + u + f32(bias[cols(k)].reshape(1, CHUNK) if row is None else bias[row:row + 1, cols(k)])).astype(BF)
            self.x[rows, cols(k)] = new
            v = f32(new)
            self.ss[rows, :] += fold_lanes(v * v)

        return update

    def all_reduce(self, bias, row):
        par = self.n_ar % 2
        self.n_ar += 1
        self.ss[...] = jnp.zeros_like(self.ss)
        self.comm.finish(par, self.updater(bias, row))

    def down(self, phase, depth, per_chunk, lhs):
        st, comm, par = self.stream, self.comm, self.n_ar % 2
        start = phase[0]
        ahead = start + st.n_slots
        stop = ahead + per_chunk * N_CHUNK

        @pl.loop(0, N_CHUNK)
        def _(k):
            for h in range(2):
                if per_chunk == 2 or h == 0:
                    slot = st.wait(phase, k * per_chunk + h)
                off = 0 if per_chunk == 2 else h * depth
                prod = jnp.dot(lhs[...], st.slots[slot, off:off + depth, :], preferred_element_type=F32).astype(BF)
                for r in range(2):
                    comm.part[k, r, :, h * TILE:(h + 1) * TILE] = prod[r * HALF:(r + 1) * HALF]
            for h in range(per_chunk):
                st.issue(ahead + k * per_chunk + h, ahead, stop)
            comm.copy1(par, k).start()

            @pl.when(k >= 1)
            def _():
                comm.chip_sum(par, k - 1)

        comm.chip_sum(par, N_CHUNK - 1)

    def mlp(self, up, down, layer, b1, b2, bd):
        st = self.stream
        start = up[0]
        ahead = start + st.n_slots
        stop = ahead + 24

        @pl.loop(0, 6)
        def _(q):
            got = [st.wait(up, 4 * q + h) for h in range(4)]
            dots = [jnp.dot(self.n[...], st.slots[slot], preferred_element_type=F32) for slot in got]
            for h in range(4):
                st.issue(ahead + 4 * q + h, ahead, stop)
            for h in range(2):
                c = cols(2 * q + h, TILE)
                gate = dots[2 * h] + f32(b1[layer:layer + 1, c])
                lin = dots[2 * h + 1] + f32(b2[layer:layer + 1, c])
                self.hid[:, c] = (gelu(gate) * lin).astype(BF)

        self.down(down, 3072, 2, self.hid)
        self.all_reduce(bd, layer)


    def recurrent(self, x_tiles, mixed, y_tiles, out_tiles, layer, v, outs):
        st = self.stream
        ahead = x_tiles[0] + st.n_slots
        stop = ahead + 11

        def dots(phase, tiles):
            slots = [st.wait(phase, i) for i in tiles]
            return [jnp.dot(self.n[...], st.slots[slot], preferred_element_type=F32) for slot in slots]

        def put_x(i, g):
            v.xb[:, cols(i, TILE)] = (g + f32(v.bx[layer:layer + 1, cols(i, TILE)])).astype(BF)

        @pl.loop(0, 2)
        def _(p):
            for h, g in enumerate(dots(x_tiles, [2 * p, 2 * p + 1])):
                put_x(2 * p + h, g)
            for h in range(2):
                st.issue(ahead + 2 * p + h, ahead, stop)

        if layer == 0:
            self.comm.meet()
        last_x, = dots(x_tiles, [4])
        g, = dots(mixed, [0])
        for h in range(2):
            st.issue(ahead + 4 + h, ahead, stop)
        put_x(4, last_x)
        v.xb[:, 1280:1408] = (g[:, 0:128] + f32(v.bx[layer:layer + 1, 1280:1408])).astype(BF)
        v.yg[...] = gelu(g[:, 128:256] + f32(v.by[layer:layer + 1, 1280:1408]))

        outs.wait_inputs(layer)
        pos = v.tokc[...]

        @pl.loop(0, 11)
        def _(i):
            c = cols(i, 128)
            acc = f32(v.cb[layer:layer + 1, c]) + f32(v.cw[layer, 0:1, c]) * f32(v.xb[:, c])
            for j in range(3):
                acc = acc + jnp.where(pos >= 3 - j, f32(v.conv[j, :, c]), 0.0) * f32(v.cw[layer, 3 - j:4 - j, c])
            v.xc[:, c] = acc.astype(BF)

        for b in range(8):
            c = slice(176 * b, 176 * (b + 1))
            xc = v.xc[:, c]
            v.rp[:, c] = jnp.dot(xc, v.ga[b], preferred_element_type=F32)
            v.ip[:, c] = jnp.dot(xc, v.gi[b], preferred_element_type=F32)

        def gate(c, reset):
            rate = -8.0 * jax.nn.softplus(v.ap[layer:layer + 1, c])
            decay = jnp.exp(rate * jax.nn.sigmoid(v.rp[:, c] + f32(v.gba[layer:layer + 1, c])))
            into = jnp.sqrt(1.0 - decay * decay)
            decay = jnp.where(reset, 0.0, decay)
            into = jnp.where(reset, 1.0, into)
            new = decay * v.lru[:, c] + into * jax.nn.sigmoid(v.ip[:, c] + f32(v.gbi[layer:layer + 1, c])) * f32(v.xc[:, c])
            v.lru[:, c] = new
            return new

        def put_y(i, g):
            for h in range(2):
                c = cols(2 * i + h, 128)
                new = gate(c, pos == 0)
                y = gelu(g[:, 128 * h:128 * (h + 1)] + f32(v.by[layer:layer + 1, c]))
                v.gated[:, c] = (new * y).astype(BF)

        @pl.loop(0, 2)
        def _(p):
            for h, g in enumerate(dots(y_tiles, [2 * p, 2 * p + 1])):
                put_y(2 * p + h, g)
            for h in range(2):
                st.issue(ahead + 6 + 2 * p + h, ahead, stop)

        g, = dots(y_tiles, [4])
        st.issue(ahead + 10, ahead, stop)
        put_y(4, g)
        c = slice(1280, 1408)
        v.gated[:, c] = (gate(c, pos == 0) * v.yg[...]).astype(BF)
        outs.write(layer)
        self.down(out_tiles, 1408, 1, v.gated)
        self.all_reduce(v.bout, layer)
        outs.wait_write(layer)
        if layer == 0:
            outs.start_inputs(1)


def add_mlp(stream, w1, w2, wd, layer):
    up = stream.add(24, columns(w1, layer, D), columns(w2, layer, D))
    return up, stream.add(16, columns(wd, layer, 3072))


class Names:
    def __init__(self, **kw):
        self.__dict__.update(kw)


class StateCopies:
    def __init__(self, ins, xb_out, lru_out, v, in_sem, out_sem):
        self.ins, self.xb_out, self.lru_out, self.v, self.in_sem, self.out_sem = ins, xb_out, lru_out, v, in_sem, out_sem

    def inputs(self, layer):
        return [pltpu.make_async_copy(src.at[layer], dst, self.in_sem.at[layer, i]) for i, (src, dst) in enumerate(self.ins)]

    def start_inputs(self, layer):
        for c in self.inputs(layer):
            c.start()

    def wait_inputs(self, layer):
        for c in self.inputs(layer):
            c.wait()

    def outputs(self, layer):
        pairs = [(self.v.xb, self.xb_out.at[layer]), (self.v.lru, self.lru_out.at[layer])]
        return [pltpu.make_async_copy(src, dst, self.out_sem.at[layer, i]) for i, (src, dst) in enumerate(pairs)]

    def write(self, layer):
        for c in self.outputs(layer):
            c.start()

    def wait_write(self, layer):
        for c in self.outputs(layer):
            c.wait()


N_SLOTS_A = 19
WINDOW = 1024
HEADS = 8
N_COMM = 12
N_SMALL = 15
LEFT = pl.ds(0, 128)
RIGHT = pl.ds(128, 128)
FREQ = np.zeros((1, 128), np.float32)
FREQ[0, :32] = FREQ[0, 32:64] = np.float32(ROPE_BASE) ** (-np.arange(32, dtype=np.float32) / 32)


def copies(pairs, sem):
    return [pltpu.make_async_copy(a, b, sem.at[i]) for i, (a, b) in enumerate(pairs)]


def start(group):
    for c in group:
        c.start()


def finish(group):
    for c in group:
        c.wait()


N_SLOTS_B = 22
N_SLOTS_C = 23

COMM_SCRATCH = [
    pltpu.VMEM((N_CHUNK, 2, HALF, CHUNK), BF), pltpu.VMEM((N_CHUNK, HALF, CHUNK), BF), pltpu.VMEM((N_CHUNK, HALF, CHUNK), BF),
    pltpu.VMEM((2, N_CHUNK, HALF, CHUNK), BF), pltpu.VMEM((N_CHUNK, HALF, CHUNK), BF), pltpu.VMEM((N_CHUNK, HALF, CHUNK), BF),
] + [pltpu.SemaphoreType.DMA((2, N_CHUNK)) for _ in range(6)]


def body_scratch(n_slots, n_pieces):
    return [pltpu.VMEM((n_slots, D, TILE), BF), pltpu.SemaphoreType.DMA((n_slots, n_pieces)), pltpu.VMEM((ROWS, D), BF), pltpu.VMEM((ROWS, D), BF)]


def recurrent_kernel(tok, x_in, conv, lru, nscale, wx, bx, wy, by, cw, cb, ga, gba, gi, gbi, ap, wout, bout, w1, b1, w2, b2, wd, bd, freq, wq, wk, wv, *refs):
    (x_out, xb_out, lru_out, q_out, k_row, v_row), refs = refs[:6], refs[6:]
    (slots, sems, x, n, hid, ss), refs = refs[:6], refs[6:]
    comm = Comm(*refs[:N_COMM])
    refs = refs[N_COMM:]
    small, refs = refs[:N_SMALL], refs[N_SMALL:]
    v_tok, v_ns, v_bx, v_by, v_cw, v_cb, v_gba, v_gbi, v_ap, v_bout, v_b1, v_b2, v_bd, v_freq, small_sem = small
    v_conv, v_lru, v_ga, v_gi, xb, yg, xc, rp, ip, gated, tokc, q3, k_new, v_new, v_cos, v_sin, in_sem, out_sem, row_sem = refs
    stream = Stream(slots, sems, N_SLOTS_A)
    v = Names(bx=v_bx, by=v_by, cw=v_cw, cb=v_cb, ga=v_ga, gba=v_gba, gi=v_gi, gbi=v_gbi, ap=v_ap, bout=v_bout, conv=v_conv, lru=v_lru, xb=xb, yg=yg, xc=xc, rp=rp, ip=ip, gated=gated, tokc=tokc)
    outs = StateCopies([(conv, v_conv), (lru, v_lru), (ga, v_ga), (gi, v_gi)], xb_out, lru_out, v, in_sem, out_sem)
    body = Body(stream, comm, x, n, hid, ss, v_ns)

    plan = []
    for layer in range(2):
        xt = stream.add(5, columns(wx, layer, D))
        mixed = stream.add(1, lambda j, layer=layer: [(wx.at[layer, :, 1280:1408], (pl.ds(0, D), pl.ds(0, 128))), (wy.at[layer, :, 1280:1408], (pl.ds(0, D), pl.ds(128, 128)))])
        yt = stream.add(5, columns(wy, layer, D))
        ot = stream.add(8, lambda j, layer=layer: [(wout.at[layer, :, pl.ds(pl.multiple_of(j * CHUNK + h * TILE, TILE), TILE)], (pl.ds(h * 1408, 1408), pl.ds(0, TILE))) for h in range(2)])
        up, down = add_mlp(stream, w1, w2, wd, layer)
        plan.append((xt, mixed, yt, ot, up, down))
    qt = stream.add(4, lambda j: [(wq.at[:, cols(j, TILE)], full(D))])
    kvt = stream.add(1, lambda j: [(wk, (pl.ds(0, D), LEFT)), (wv, (pl.ds(0, D), RIGHT))])

    pairs = [(x_in, x), (tok, v_tok), (nscale, v_ns), (bx, v_bx), (by, v_by), (cw, v_cw), (cb, v_cb), (gba, v_gba), (gbi, v_gbi), (ap, v_ap), (bout, v_bout), (b1, v_b1), (b2, v_b2), (bd, v_bd), (freq, v_freq)]
    early = copies(pairs, small_sem)
    start(early)
    comm.greet()
    stream.prime(0, 6)
    outs.start_inputs(0)
    stream.prime(6, N_SLOTS_A)
    for c in early:
        c.wait()
    tokc[...] = jnp.broadcast_to(v_tok[...], (ROWS, 128)).T
    body.squares()
    for layer in range(2):
        xt, mixed, yt, ot, up, down = plan[layer]
        body.norm(2 * layer)
        body.recurrent(xt, mixed, yt, ot, layer, v, outs)
        body.norm(2 * layer + 1)
        body.mlp(up, down, layer, v_b1, v_b2, v_bd)
    last = pltpu.make_async_copy(x, x_out, small_sem.at[0])
    last.start()
    body.norm(4)
    lane = lax.broadcasted_iota(jnp.int32, (ROWS, 128), 1)
    angle = f32(tokc[...]) * v_freq[...]
    v_cos[...] = jnp.cos(angle)
    v_sin[...] = jnp.sin(angle) * jnp.where(lane < 32, -1.0, 1.0)

    def rope(val):
        other = jnp.where(lane < 32, pltpu.roll(val, 96, 1), pltpu.roll(val, 32, 1))
        return f32((val * v_cos[...] + other * v_sin[...]).astype(BF))

    @pl.loop(0, 2)
    def _(p):
        got = [stream.wait(qt, 2 * p + i) for i in range(2)]
        for i, slot in enumerate(got):
            g = jnp.dot(n[...], slots[slot], preferred_element_type=F32)
            for h in range(2):
                q3[pl.ds(4 * p + 2 * i + h, ROWS, stride=HEADS), :] = rope(g[:, 128 * h:128 * (h + 1)])

    slot = stream.wait(kvt, 0)
    g = jnp.dot(n[...], slots[slot], preferred_element_type=F32)
    k_new[...] = rope(g[:, :128])
    v_new[...] = f32(g[:, 128:].astype(BF))
    rows = copies([(q3, q_out), (k_new, k_row), (v_new, v_row)], row_sem)
    start(rows)
    finish(rows)
    last.wait()


def final_kernel(x_in, o_in, nscale, bo, wo, w1, b1, w2, b2, wd, bd, *refs):
    (x, slots, sems, n, hid, ss), refs = refs[:6], refs[6:]
    comm = Comm(*refs[:N_COMM])
    v_ns, v_bo, v_b1, v_b2, v_bd, o3, o_bf, small_sem = refs[N_COMM:]
    stream = Stream(slots, sems, N_SLOTS_C)
    body = Body(stream, comm, x, n, hid, ss, v_ns)
    ot = stream.add(8, lambda j: [(wo.at[:, pl.ds(pl.multiple_of(j * CHUNK + h * TILE, TILE), TILE)], (pl.ds(h * WINDOW, WINDOW), pl.ds(0, TILE))) for h in range(2)])
    up, down = add_mlp(stream, w1, w2, wd, 2)
    early = copies([(o_in, o3), (x_in, x), (nscale, v_ns), (bo, v_bo), (b1, v_b1), (b2, v_b2), (bd, v_bd)], small_sem)
    start(early)
    comm.greet()
    stream.prime(0, N_SLOTS_C)
    finish(early)
    for h in range(HEADS):
        o_bf[:, 128 * h:128 * (h + 1)] = o3[pl.ds(h, ROWS, stride=HEADS), :].astype(BF)
    comm.meet()
    body.down(ot, WINDOW, 1, o_bf)
    body.all_reduce(v_bo, None)
    body.norm(5)
    body.mlp(up, down, 2, v_b1, v_b2, v_bd)


GROUP = 4
N_GROUP = ROWS // GROUP
LAG = 4


def attention_kernel(pos_s, tok, q_in, k_row, v_row, conv, xb, lru, k_cache, v_cache, slot_pos, o_out, conv_out, lru_out, k_out, v_out, slot_out,
                     slots, sems, v_tok, v_conv, v_lru, v_slot, bias, q3, o3, k_new, v_new, small_sem, state_sem, out_sem):
    stream = Stream(slots, sems, N_SLOTS_B)

    def group_rows(j):
        return pl.ds(pl.multiple_of(j * GROUP * WINDOW, GROUP * WINDOW), GROUP * WINDOW)

    ct = stream.add(N_GROUP, lambda j: [(src.at[group_rows(j)], (pl.ds(0, D), part)) for part, src in ((LEFT, k_cache), (RIGHT, v_cache))])
    early = copies([(tok, v_tok), (slot_pos, v_slot), (q_in, q3), (k_row, k_new), (v_row, v_new)], small_sem)
    start(early)
    stream.prime(0, N_SLOTS_B // 2)
    states = copies([(conv.at[:, 1:3], v_conv.at[:, 0:2]), (xb, v_conv.at[:, 2]), (lru, v_lru)], state_sem)
    start(states)
    stream.prime(N_SLOTS_B // 2, N_SLOTS_B)
    finish(early)
    pos = jnp.broadcast_to(v_tok[...], (ROWS, 128)).T
    target = lax.rem(pos, WINDOW)
    lane = lax.broadcasted_iota(jnp.int32, (ROWS, 128), 1)

    @pl.loop(0, WINDOW // 128)
    def _(i):
        now = jnp.where(lane + i * 128 == target, pos, v_slot[:, cols(i, 128)])
        v_slot[:, cols(i, 128)] = now
        age = pos - now
        good = (now >= 0) & (age >= 0) & (age < WINDOW)
        bias[:, cols(i, 128)] = jnp.where(good, 0.0, -jnp.inf)

    results = copies([(v_conv, conv_out), (v_lru, lru_out), (v_slot, slot_out)], state_sem)

    def outputs(j):
        slot = stream.slot_of(ct[0] + j)
        return [pltpu.make_async_copy(slots.at[slot, :, pl.ds(128 * i, 128)], dst.at[group_rows(j)], out_sem.at[slot, i]) for i, dst in enumerate((k_out, v_out))]

    row16 = lax.broadcasted_iota(jnp.int32, (16, 128), 0)
    ahead = ct[0] - LAG + stream.n_slots
    nt = (((1,), (1,)), ((), ()))

    @pl.loop(0, N_GROUP // 2)
    def _(p):
        got = [stream.wait(ct, 2 * p + g) for g in range(2)]
        for g, slot in enumerate(got):
            for r in range(GROUP):
                seq = (2 * p + g) * GROUP + r
                spot = lax.rem(pos_s[seq], WINDOW)
                base = pl.multiple_of(r * WINDOW + lax.div(spot, 16) * 16, 16)
                for i, new in enumerate((k_new, v_new)):
                    here = (slot, pl.ds(base, 16), pl.ds(128 * i, 128))
                    slots[here] = jnp.where(row16 == lax.rem(spot, 16), new[pl.ds(seq, 1), :], f32(slots[here])).astype(BF)
            start(outputs(2 * p + g))

        pairs = [(slot, h) for slot in got for h in range(GROUP // 2)]
        first = 2 * p * GROUP
        scores = []
        for i, (slot, h) in enumerate(pairs):
            q = q3[pl.ds(pl.multiple_of((first + 2 * i) * HEADS, 2 * HEADS), 2 * HEADS), :].astype(BF)
            halves = []
            for e in range(2):
                r = 2 * h + e
                keys = slots[slot, r * WINDOW:(r + 1) * WINDOW, 0:128]
                score = lax.dot_general(q, keys, nt, preferred_element_type=F32)[HEADS * e:HEADS * (e + 1)] * (128 ** -0.5)
                halves.append(score + bias[pl.ds(first + 2 * i + e, 1), :])
            scores.append(jnp.concatenate(halves, axis=0))
        probs = []
        for score in scores:
            e = jnp.exp(score - jnp.max(score, axis=-1, keepdims=True))
            probs.append((e / jnp.sum(e, axis=-1, keepdims=True)).astype(BF))
        for i, (slot, h) in enumerate(pairs):
            halves = []
            for e in range(2):
                r = 2 * h + e
                values = slots[slot, r * WINDOW:(r + 1) * WINDOW, 128:256]
                halves.append(jnp.dot(probs[i], values, preferred_element_type=F32)[HEADS * e:HEADS * (e + 1)])
            o3[pl.ds(pl.multiple_of((first + 2 * i) * HEADS, 2 * HEADS), 2 * HEADS), :] = jnp.concatenate(halves, axis=0)

        @pl.when(2 * p >= LAG)
        def _():
            @pl.when(2 * p == LAG)
            def _():
                finish(states)
                start(results)

            for g in range(2):
                finish(outputs(2 * p + g - LAG))
                stream.issue(ahead + 2 * p + g, ahead + LAG, ahead + N_GROUP)

    last = pltpu.make_async_copy(o3, o_out, small_sem.at[0])
    last.start()
    for j in range(N_GROUP - LAG, N_GROUP):
        finish(outputs(j))
    finish(results)
    last.wait()


ANY = pl.BlockSpec(memory_space=pl.ANY)


def io_specs():
    in_specs = (P('dp', None), P('dp'), P(None, 'dp', None, 'tp'), P(None, 'dp', 'tp'), P('dp', None, None), P('dp', None, None), P('dp', None),
                P(), P(None, None, 'tp'), P(None, 'tp'), P(None, None, 'tp'), P(None, 'tp'), P(None, None, 'tp'), P(None, 'tp'),
                P(None, 'tp', None, None), P(None, 'tp'), P(None, 'tp', None, None), P(None, 'tp'), P(None, 'tp'), P(None, 'tp', None), P(),
                P(None, 'tp'), P(), P(), P('tp', None), P(),
                P(None, None, 'tp'), P(None, 'tp'), P(None, None, 'tp'), P(None, 'tp'), P(None, 'tp', None), P())
    out_specs = (P('dp', None), P(None, 'dp', None, 'tp'), P(None, 'dp', 'tp'), P('dp', None, None), P('dp', None, None), P('dp', None))
    return in_specs, out_specs


def solution(mesh):
    in_specs, out_specs = io_specs()
    shape = jax.ShapeDtypeStruct

    def local_step(x_in, tok_pos, conv_state, lru_state, k_cache, v_cache, slot_pos, norm_scale, rec_wx, rec_bx, rec_wy, rec_by, conv_w, conv_b, gate_wa, gate_ba, gate_wi, gate_bi, a_param, rec_wout, rec_bout, attn_wq, attn_wk, attn_wv, attn_wo, attn_bo, mlp_w1, mlp_b1, mlp_w2, mlp_b2, mlp_wd, mlp_bd):
        tok = tok_pos.reshape(1, ROWS)
        conv_t = jnp.transpose(conv_state, (0, 2, 1, 3))
        vec, vec_f = pltpu.VMEM((2, LOCAL), BF), pltpu.VMEM((2, LOCAL), F32)
        wide, wide_f = pltpu.VMEM((ROWS, LOCAL), BF), pltpu.VMEM((ROWS, LOCAL), F32)
        table, gates, heads = pltpu.VMEM((ROWS, 128), F32), pltpu.VMEM((8, 176, 176), BF), pltpu.VMEM((ROWS * HEADS, 128), F32)
        scale, mlp_b, pos_row, freq = pltpu.VMEM((3, 2, D), BF), pltpu.VMEM((3, 3072), BF), pltpu.VMEM((1, ROWS), jnp.int32), jnp.asarray(FREQ)
        hidden, out_b = pltpu.VMEM((ROWS, 3072), BF), pltpu.VMEM((3, D), BF)
        dma = pltpu.SemaphoreType.DMA
        row, head_rows, branch, state = shape((ROWS, 128), F32), shape((ROWS * HEADS, 128), F32), shape((2, ROWS, LOCAL), BF), shape((2, ROWS, LOCAL), F32)
        x_mid, xb, lru_mid, q_rows, k_row, v_row = pl.pallas_call(
            recurrent_kernel,
            out_shape=[shape((ROWS, D), BF), branch, state, head_rows, row, row],
            in_specs=[ANY] * 28, out_specs=[ANY] * 6,
            scratch_shapes=body_scratch(N_SLOTS_A, 2) + [hidden, table] + COMM_SCRATCH + [
                pos_row, scale, vec, vec, pltpu.VMEM((2, 4, LOCAL), BF), vec, vec, vec, vec_f, pltpu.VMEM((2, D), BF), mlp_b, mlp_b, out_b, pltpu.VMEM((1, 128), F32), dma((N_SMALL,)),
                pltpu.VMEM((3, ROWS, LOCAL), BF), wide_f, gates, gates, wide, table, wide, wide_f, wide_f, wide, pltpu.VMEM((ROWS, 128), jnp.int32),
                heads, table, table, table, table, dma((2, 4)), dma((2, 2)), dma((3,))],
            compiler_params=pltpu.CompilerParams(collective_id=0, has_side_effects=True, vmem_limit_bytes=VMEM_LIMIT),
            name='recurrent_layers',
        )(tok, x_in, conv_t, lru_state, norm_scale, rec_wx, rec_bx, rec_wy, rec_by, conv_w, conv_b, gate_wa, gate_ba, gate_wi, gate_bi, a_param, rec_wout, rec_bout, mlp_w1, mlp_b1, mlp_w2, mlp_b2, mlp_wd, mlp_bd, freq, attn_wq, attn_wk, attn_wv)
        cache = (ROWS * WINDOW, 128)
        o_rows, conv_out, lru_out, k_out, v_out, slot_out = pl.pallas_call(
            attention_kernel,
            out_shape=[head_rows, shape((2, 3, ROWS, LOCAL), BF), state, shape(cache, BF), shape(cache, BF), shape((ROWS, WINDOW), jnp.int32)],
            in_specs=[pl.BlockSpec(memory_space=pltpu.SMEM)] + [ANY] * 10, out_specs=[ANY] * 6,
            scratch_shapes=body_scratch(N_SLOTS_B, 2)[:2] + [
                pos_row, pltpu.VMEM((2, 3, ROWS, LOCAL), BF), pltpu.VMEM((2, ROWS, LOCAL), F32), pltpu.VMEM((ROWS, WINDOW), jnp.int32), pltpu.VMEM((ROWS, WINDOW), F32),
                heads, heads, table, table, dma((5,)), dma((3,)), dma((N_SLOTS_B, 2))],
            compiler_params=pltpu.CompilerParams(vmem_limit_bytes=VMEM_LIMIT),
            name='attention_layer',
        )(tok_pos, tok, q_rows, k_row, v_row, conv_t, xb, lru_mid, k_cache.reshape(cache), v_cache.reshape(cache), slot_pos)
        x_out = pl.pallas_call(
            final_kernel,
            out_shape=shape((ROWS, D), BF),
            in_specs=[ANY] * 11, out_specs=pl.BlockSpec(memory_space=pltpu.VMEM),
            scratch_shapes=body_scratch(N_SLOTS_C, 2)[:3] + [hidden, table] + COMM_SCRATCH + [scale, pltpu.VMEM((D,), BF), mlp_b, mlp_b, out_b, heads, pltpu.VMEM((ROWS, WINDOW), BF), dma((7,))],
            compiler_params=pltpu.CompilerParams(collective_id=1, has_side_effects=True, vmem_limit_bytes=VMEM_LIMIT),
            name='last_mlp',
        )(x_mid, o_rows, norm_scale, attn_bo, attn_wo, mlp_w1, mlp_b1, mlp_w2, mlp_b2, mlp_wd, mlp_bd)
        return (x_out, jnp.transpose(conv_out, (0, 2, 1, 3)), lru_out, k_out.reshape(k_cache.shape), v_out.reshape(v_cache.shape), slot_out)

    return jax.shard_map(local_step, mesh=mesh, in_specs=in_specs, out_specs=out_specs, check_vma=False)
```

```python
import jax
import jax.numpy as jnp
import numpy as np
from jax import lax
from jax.experimental import pallas as pl
from jax.experimental.pallas import tpu as pltpu
from jax.sharding import PartitionSpec as P

ROPE_BASE = 10000.0
NORM_EPS = 1e-6
BF = jnp.bfloat16
F32 = jnp.float32
ROWS = 128
LOCAL = 1408
D = 4096
TILE = 256
CHUNK = 512
N_CHUNK = D // CHUNK
HALF = ROWS // 2
VMEM_LIMIT = 67043328


class Stream:
    def __init__(self, slots, sems, n_slots):
        self.slots, self.sems, self.n_slots = slots, sems, n_slots
        self.phases = []
        self.total = 0

    def add(self, n, *kinds):
        start = self.total
        self.phases.append((start, n, kinds))
        self.total += n
        return start, kinds

    def slot_of(self, t):
        return lax.rem(t, self.n_slots)

    def copies(self, kind, j, slot):
        return [pltpu.make_async_copy(src, self.slots.at[(slot,) + dst], self.sems.at[slot, i]) for i, (src, dst) in enumerate(kind(j))]

    def start_tile(self, kinds, j, slot):
        n = len(kinds)
        if n == 1:
            for c in self.copies(kinds[0], j, slot):
                c.start()
            return
        for which, kind in enumerate(kinds):
            @pl.when(lax.rem(j, n) == which)
            def _(kind=kind):
                for c in self.copies(kind, lax.div(j, n), slot):
                    c.start()

    def issue(self, t, lo, hi):
        for start, n, kinds in self.phases:
            if start + n <= lo or hi <= start:
                continue

            def go(start=start, kinds=kinds):
                self.start_tile(kinds, t - start, self.slot_of(t))

            if start <= lo and hi <= start + n:
                go()
            else:
                pl.when(jnp.logical_and(t >= start, t < start + n))(go)

    def prime(self, lo, hi):
        for start, n, kinds in self.phases:
            first, stop = max(start, lo), min(start + n, hi, self.n_slots)
            if first < stop:
                @pl.loop(first, stop)
                def _(t, start=start, kinds=kinds):
                    self.start_tile(kinds, t - start, self.slot_of(t))

    def wait(self, phase, j):
        start, kinds = phase
        slot = self.slot_of(start + j)
        for c in self.copies(kinds[0], lax.div(j, len(kinds)), slot):
            c.wait()
        return slot


def full(slot_rows):
    return (pl.ds(0, slot_rows), pl.ds(0, TILE))


def columns(ref, layer, rows):
    return lambda j: [(ref.at[layer, :, pl.ds(pl.multiple_of(j * TILE, TILE), TILE)], full(rows))]


def gelu(v):
    return jax.nn.gelu(v, approximate=True)


def f32(v):
    return v.astype(F32)


def cols(k, width=CHUNK):
    return pl.ds(pl.multiple_of(k * width, width), width)


class Comm:
    def __init__(self, part, r1, cs, r2, fin, r3, s1, q1, s2, q2, s3, q3):
        self.part, self.r1, self.cs, self.r2, self.fin, self.r3 = part, r1, cs, r2, fin, r3
        self.s1, self.q1, self.s2, self.q2, self.s3, self.q3 = s1, q1, s2, q2, s3, q3
        me = lax.axis_index('tp')
        self.mine = lax.rem(me, 2)
        self.other = 1 - self.mine
        self.partner = me + 1 - 2 * self.mine
        self.peer = lax.rem(me + 2, 4)

    def greet(self):
        for dev in (self.partner, self.peer):
            pl.semaphore_signal(pltpu.get_barrier_semaphore(), inc=1, device_id={'tp': dev}, device_id_type=pl.DeviceIdType.MESH)

    def meet(self):
        pl.semaphore_wait(pltpu.get_barrier_semaphore(), 2)

    def copy1(self, par, k):
        return pltpu.make_async_remote_copy(src_ref=self.part.at[k, self.other], dst_ref=self.r1.at[k], send_sem=self.s1.at[par, k], recv_sem=self.q1.at[par, k], device_id={'tp': self.partner}, device_id_type=pl.DeviceIdType.MESH)

    def copy2(self, par, k):
        return pltpu.make_async_remote_copy(src_ref=self.cs.at[k], dst_ref=self.r2.at[par, k], send_sem=self.s2.at[par, k], recv_sem=self.q2.at[par, k], device_id={'tp': self.peer}, device_id_type=pl.DeviceIdType.MESH)

    def copy3(self, par, k):
        return pltpu.make_async_remote_copy(src_ref=self.fin.at[k], dst_ref=self.r3.at[k], send_sem=self.s3.at[par, k], recv_sem=self.q3.at[par, k], device_id={'tp': self.partner}, device_id_type=pl.DeviceIdType.MESH)

    def chip_sum(self, par, k):
        self.copy1(par, k).wait_recv()
        self.cs[k] = (f32(self.part[k, self.mine]) + f32(self.r1[k])).astype(BF)
        self.copy2(par, k).start()

    def finish(self, par, update):
        @pl.loop(0, N_CHUNK)
        def _(k):
            self.copy2(par, k).wait_recv()
            total = (f32(self.cs[k]) + f32(self.r2[par, k])).astype(BF)
            self.fin[k] = total
            self.copy3(par, k).start()
            update(self.mine, k, f32(total))

            @pl.when(k >= 1)
            def _():
                self.copy3(par, k - 1).wait_recv()
                update(self.other, k - 1, f32(self.r3[k - 1]))

        self.copy3(par, N_CHUNK - 1).wait_recv()
        update(self.other, N_CHUNK - 1, f32(self.r3[N_CHUNK - 1]))

    def sent(self, par):
        @pl.loop(0, N_CHUNK)
        def _(k):
            self.copy1(par, k).wait_send()
            self.copy2(par, k).wait_send()
            self.copy3(par, k).wait_send()


def fold_lanes(v):
    acc = v[:, 0:128]
    for i in range(1, v.shape[1] // 128):
        acc = acc + v[:, 128 * i:128 * (i + 1)]
    return acc


class Body:
    def __init__(self, stream, comm, x, n, hid, ss, nscale):
        self.stream, self.comm, self.x, self.n, self.hid, self.ss, self.nscale = stream, comm, x, n, hid, ss, nscale
        self.n_ar = 0

    def squares(self):
        self.ss[...] = jnp.zeros_like(self.ss)

        @pl.loop(0, N_CHUNK)
        def _(k):
            v = f32(self.x[:, cols(k)])
            self.ss[...] += fold_lanes(v * v)

    def norm(self, row):
        scale = lax.rsqrt(jnp.sum(self.ss[...], axis=-1, keepdims=True) * (1.0 / D) + NORM_EPS)

        @pl.loop(0, N_CHUNK)
        def _(k):
            gain = 1.0 + f32(self.nscale[row // 2, row % 2:row % 2 + 1, cols(k)])
            self.n[:, cols(k)] = (f32(self.x[:, cols(k)]) * scale * gain).astype(BF)

        if self.n_ar:
            self.comm.sent((self.n_ar - 1) % 2)

    def updater(self, bias, row):
        def update(half, k, u):
            rows = pl.ds(pl.multiple_of(half * HALF, HALF), HALF)
            new = (f32(self.x[rows, cols(k)]) + u + f32(bias[cols(k)].reshape(1, CHUNK) if row is None else bias[row:row + 1, cols(k)])).astype(BF)
            self.x[rows, cols(k)] = new
            v = f32(new)
            self.ss[rows, :] += fold_lanes(v * v)

        return update

    def all_reduce(self, bias, row):
        par = self.n_ar % 2
        self.n_ar += 1
        self.ss[...] = jnp.zeros_like(self.ss)
        self.comm.finish(par, self.updater(bias, row))

    def down(self, phase, depth, per_chunk, lhs):
        st, comm, par = self.stream, self.comm, self.n_ar % 2
        start = phase[0]
        ahead = start + st.n_slots
        stop = ahead + per_chunk * N_CHUNK

        @pl.loop(0, N_CHUNK)
        def _(k):
            for h in range(2):
                if per_chunk == 2 or h == 0:
                    slot = st.wait(phase, k * per_chunk + h)
                off = 0 if per_chunk == 2 else h * depth
                prod = jnp.dot(lhs[...], st.slots[slot, off:off + depth, :], preferred_element_type=F32).astype(BF)
                for r in range(2):
                    comm.part[k, r, :, h * TILE:(h + 1) * TILE] = prod[r * HALF:(r + 1) * HALF]
            for h in range(per_chunk):
                st.issue(ahead + k * per_chunk + h, ahead, stop)
            comm.copy1(par, k).start()

            @pl.when(k >= 1)
            def _():
                comm.chip_sum(par, k - 1)

        comm.chip_sum(par, N_CHUNK - 1)

    def mlp(self, up, down, layer, b1, b2, bd):
        st = self.stream
        start = up[0]
        ahead = start + st.n_slots
        stop = ahead + 24

        @pl.loop(0, 6)
        def _(q):
            got = [st.wait(up, 4 * q + h) for h in range(4)]
            dots = [jnp.dot(self.n[...], st.slots[slot], preferred_element_type=F32) for slot in got]
            for h in range(4):
                st.issue(ahead + 4 * q + h, ahead, stop)
            for h in range(2):
                c = cols(2 * q + h, TILE)
                gate = dots[2 * h] + f32(b1[layer:layer + 1, c])
                lin = dots[2 * h + 1] + f32(b2[layer:layer + 1, c])
                self.hid[:, c] = (gelu(gate) * lin).astype(BF)

        self.down(down, 3072, 2, self.hid)
        self.all_reduce(bd, layer)


    def recurrent(self, x_tiles, mixed, y_tiles, out_tiles, layer, v, outs):
        st = self.stream
        ahead = x_tiles[0] + st.n_slots
        stop = ahead + 11

        def dots(phase, tiles):
            slots = [st.wait(phase, i) for i in tiles]
            return [jnp.dot(self.n[...], st.slots[slot], preferred_element_type=F32) for slot in slots]

        def put_x(i, g):
            v.xb[:, cols(i, TILE)] = (g + f32(v.bx[layer:layer + 1, cols(i, TILE)])).astype(BF)

        @pl.loop(0, 2)
        def _(p):
            for h, g in enumerate(dots(x_tiles, [2 * p, 2 * p + 1])):
                put_x(2 * p + h, g)
            for h in range(2):
                st.issue(ahead + 2 * p + h, ahead, stop)

        outs.wait_inputs(layer)
        pos = v.tokc[...]

        def conv(i):
            c = slice(128 * i, 128 * (i + 1))
            acc = f32(v.cb[layer:layer + 1, c]) + f32(v.cw[layer, 0:1, c]) * f32(v.xb[:, c])
            for j in range(3):
                acc = acc + jnp.where(pos >= 3 - j, f32(v.conv[j, :, c]), 0.0) * f32(v.cw[layer, 3 - j:4 - j, c])
            v.xc[:, c] = acc.astype(BF)

        if layer == 0:
            self.comm.meet()
        slots = [st.wait(x_tiles, 4), st.wait(mixed, 0)]
        last_x, g = [jnp.dot(self.n[...], st.slots[slot], preferred_element_type=F32) for slot in slots]
        for i in range(8):
            conv(i)
        put_x(4, last_x)
        v.xb[:, 1280:] = (g[:, :128] + f32(v.bx[layer:layer + 1, 1280:])).astype(BF)
        v.yg[...] = gelu(g[:, 128:] + f32(v.by[layer:layer + 1, 1280:]))
        for h in range(2):
            st.issue(ahead + 4 + h, ahead, stop)

        first_y, = dots(y_tiles, [0])
        for i in range(8, 11):
            conv(i)
        for b in range(8):
            c = slice(176 * b, 176 * (b + 1))
            xc = v.xc[:, c]
            v.rp[:, c] = jnp.dot(xc, v.ga[b], preferred_element_type=F32)
            v.ip[:, c] = jnp.dot(xc, v.gi[b], preferred_element_type=F32)

        def gate(c, reset):
            rate = -8.0 * jax.nn.softplus(v.ap[layer:layer + 1, c])
            decay = jnp.exp(rate * jax.nn.sigmoid(v.rp[:, c] + f32(v.gba[layer:layer + 1, c])))
            into = jnp.sqrt(1.0 - decay * decay)
            decay = jnp.where(reset, 0.0, decay)
            into = jnp.where(reset, 1.0, into)
            new = decay * v.lru[:, c] + into * jax.nn.sigmoid(v.ip[:, c] + f32(v.gbi[layer:layer + 1, c])) * f32(v.xc[:, c])
            v.lru[:, c] = new
            return new

        def put_y(i, g):
            for h in range(2):
                c = cols(2 * i + h, 128)
                new = gate(c, pos == 0)
                y = gelu(g[:, 128 * h:128 * (h + 1)] + f32(v.by[layer:layer + 1, c]))
                v.gated[:, c] = (new * y).astype(BF)

        put_y(0, first_y)
        st.issue(ahead + 6, ahead, stop)

        @pl.loop(0, 2)
        def _(p):
            for h, g in enumerate(dots(y_tiles, [2 * p + 1, 2 * p + 2])):
                put_y(2 * p + 1 + h, g)
            for h in range(2):
                st.issue(ahead + 7 + 2 * p + h, ahead, stop)

        c = slice(1280, 1408)
        v.gated[:, c] = (gate(c, pos == 0) * v.yg[...]).astype(BF)
        outs.write(layer)
        self.down(out_tiles, 1408, 1, v.gated)
        self.all_reduce(v.bout, layer)
        outs.wait_write(layer)
        if layer == 0:
            outs.start_inputs(1)


def add_mlp(stream, w1, w2, wd, layer):
    up = stream.add(24, columns(w1, layer, D), columns(w2, layer, D))
    return up, stream.add(16, columns(wd, layer, 3072))


class Names:
    def __init__(self, **kw):
        self.__dict__.update(kw)


class StateCopies:
    def __init__(self, ins, xb_out, lru_out, v, in_sem, out_sem):
        self.ins, self.xb_out, self.lru_out, self.v, self.in_sem, self.out_sem = ins, xb_out, lru_out, v, in_sem, out_sem

    def inputs(self, layer):
        return [pltpu.make_async_copy(src.at[layer], dst, self.in_sem.at[layer, i]) for i, (src, dst) in enumerate(self.ins)]

    def start_inputs(self, layer):
        for c in self.inputs(layer):
            c.start()

    def wait_inputs(self, layer):
        for c in self.inputs(layer):
            c.wait()

    def outputs(self, layer):
        pairs = [(self.v.xb, self.xb_out.at[layer]), (self.v.lru, self.lru_out.at[layer])]
        return [pltpu.make_async_copy(src, dst, self.out_sem.at[layer, i]) for i, (src, dst) in enumerate(pairs)]

    def write(self, layer):
        for c in self.outputs(layer):
            c.start()

    def wait_write(self, layer):
        for c in self.outputs(layer):
            c.wait()


N_SLOTS_A = 19
WINDOW = 1024
HEADS = 8
N_COMM = 12
N_SMALL = 15
LEFT = pl.ds(0, 128)
RIGHT = pl.ds(128, 128)
FREQ = np.zeros((1, 128), np.float32)
FREQ[0, :32] = FREQ[0, 32:64] = np.float32(ROPE_BASE) ** (-np.arange(32, dtype=np.float32) / 32)


def copies(pairs, sem):
    return [pltpu.make_async_copy(a, b, sem.at[i]) for i, (a, b) in enumerate(pairs)]


def start(group):
    for c in group:
        c.start()


def finish(group):
    for c in group:
        c.wait()


N_SLOTS_B = 22
N_SLOTS_C = 23

COMM_SCRATCH = [
    pltpu.VMEM((N_CHUNK, 2, HALF, CHUNK), BF), pltpu.VMEM((N_CHUNK, HALF, CHUNK), BF), pltpu.VMEM((N_CHUNK, HALF, CHUNK), BF),
    pltpu.VMEM((2, N_CHUNK, HALF, CHUNK), BF), pltpu.VMEM((N_CHUNK, HALF, CHUNK), BF), pltpu.VMEM((N_CHUNK, HALF, CHUNK), BF),
] + [pltpu.SemaphoreType.DMA((2, N_CHUNK)) for _ in range(6)]


def body_scratch(n_slots, n_pieces):
    return [pltpu.VMEM((n_slots, D, TILE), BF), pltpu.SemaphoreType.DMA((n_slots, n_pieces)), pltpu.VMEM((ROWS, D), BF), pltpu.VMEM((ROWS, D), BF)]


def recurrent_kernel(tok, x_in, conv, lru, nscale, wx, bx, wy, by, cw, cb, ga, gba, gi, gbi, ap, wout, bout, w1, b1, w2, b2, wd, bd, freq, wq, wk, wv, *refs):
    (x_out, xb_out, lru_out, q_out, k_row, v_row), refs = refs[:6], refs[6:]
    (slots, sems, x, n, hid, ss), refs = refs[:6], refs[6:]
    comm = Comm(*refs[:N_COMM])
    refs = refs[N_COMM:]
    small, refs = refs[:N_SMALL], refs[N_SMALL:]
    v_tok, v_ns, v_bx, v_by, v_cw, v_cb, v_gba, v_gbi, v_ap, v_bout, v_b1, v_b2, v_bd, v_freq, small_sem = small
    v_conv, v_lru, v_ga, v_gi, xb, yg, xc, rp, ip, gated, tokc, q3, k_new, v_new, v_cos, v_sin, in_sem, out_sem, row_sem = refs
    stream = Stream(slots, sems, N_SLOTS_A)
    v = Names(bx=v_bx, by=v_by, cw=v_cw, cb=v_cb, ga=v_ga, gba=v_gba, gi=v_gi, gbi=v_gbi, ap=v_ap, bout=v_bout, conv=v_conv, lru=v_lru, xb=xb, yg=yg, xc=xc, rp=rp, ip=ip, gated=gated, tokc=tokc)
    outs = StateCopies([(conv, v_conv), (lru, v_lru), (ga, v_ga), (gi, v_gi)], xb_out, lru_out, v, in_sem, out_sem)
    body = Body(stream, comm, x, n, hid, ss, v_ns)

    plan = []
    for layer in range(2):
        xt = stream.add(5, columns(wx, layer, D))
        mixed = stream.add(1, lambda j, layer=layer: [(wx.at[layer, :, 1280:1408], (pl.ds(0, D), pl.ds(0, 128))), (wy.at[layer, :, 1280:1408], (pl.ds(0, D), pl.ds(128, 128)))])
        yt = stream.add(5, columns(wy, layer, D))
        ot = stream.add(8, lambda j, layer=layer: [(wout.at[layer, :, pl.ds(pl.multiple_of(j * CHUNK + h * TILE, TILE), TILE)], (pl.ds(h * 1408, 1408), pl.ds(0, TILE))) for h in range(2)])
        up, down = add_mlp(stream, w1, w2, wd, layer)
        plan.append((xt, mixed, yt, ot, up, down))
    qt = stream.add(4, lambda j: [(wq.at[:, cols(j, TILE)], full(D))])
    kvt = stream.add(1, lambda j: [(wk, (pl.ds(0, D), LEFT)), (wv, (pl.ds(0, D), RIGHT))])

    pairs = [(x_in, x), (tok, v_tok), (nscale, v_ns), (bx, v_bx), (by, v_by), (cw, v_cw), (cb, v_cb), (gba, v_gba), (gbi, v_gbi), (ap, v_ap), (bout, v_bout), (b1, v_b1), (b2, v_b2), (bd, v_bd), (freq, v_freq)]
    early = copies(pairs, small_sem)
    start(early)
    comm.greet()
    stream.prime(0, 6)
    outs.start_inputs(0)
    stream.prime(6, N_SLOTS_A)
    for c in early:
        c.wait()
    tokc[...] = jnp.broadcast_to(v_tok[...], (ROWS, 128)).T
    body.squares()
    for layer in range(2):
        xt, mixed, yt, ot, up, down = plan[layer]
        body.norm(2 * layer)
        body.recurrent(xt, mixed, yt, ot, layer, v, outs)
        body.norm(2 * layer + 1)
        body.mlp(up, down, layer, v_b1, v_b2, v_bd)
    last = pltpu.make_async_copy(x, x_out, small_sem.at[0])
    last.start()
    body.norm(4)
    lane = lax.broadcasted_iota(jnp.int32, (ROWS, 128), 1)
    angle = f32(tokc[...]) * v_freq[...]
    v_cos[...] = jnp.cos(angle)
    v_sin[...] = jnp.sin(angle) * jnp.where(lane < 32, -1.0, 1.0)

    def rope(val):
        other = jnp.where(lane < 32, pltpu.roll(val, 96, 1), pltpu.roll(val, 32, 1))
        return f32((val * v_cos[...] + other * v_sin[...]).astype(BF))

    @pl.loop(0, 2)
    def _(p):
        got = [stream.wait(qt, 2 * p + i) for i in range(2)]
        for i, slot in enumerate(got):
            g = jnp.dot(n[...], slots[slot], preferred_element_type=F32)
            for h in range(2):
                q3[pl.ds(4 * p + 2 * i + h, ROWS, stride=HEADS), :] = rope(g[:, 128 * h:128 * (h + 1)])

    slot = stream.wait(kvt, 0)
    g = jnp.dot(n[...], slots[slot], preferred_element_type=F32)
    k_new[...] = rope(g[:, :128])
    v_new[...] = f32(g[:, 128:].astype(BF))
    rows = copies([(q3, q_out), (k_new, k_row), (v_new, v_row)], row_sem)
    start(rows)
    finish(rows)
    last.wait()


def final_kernel(x_in, o_in, nscale, bo, wo, w1, b1, w2, b2, wd, bd, *refs):
    (x, slots, sems, n, hid, ss), refs = refs[:6], refs[6:]
    comm = Comm(*refs[:N_COMM])
    v_ns, v_bo, v_b1, v_b2, v_bd, o3, o_bf, small_sem = refs[N_COMM:]
    stream = Stream(slots, sems, N_SLOTS_C)
    body = Body(stream, comm, x, n, hid, ss, v_ns)
    ot = stream.add(8, lambda j: [(wo.at[:, pl.ds(pl.multiple_of(j * CHUNK + h * TILE, TILE), TILE)], (pl.ds(h * WINDOW, WINDOW), pl.ds(0, TILE))) for h in range(2)])
    up, down = add_mlp(stream, w1, w2, wd, 2)
    early = copies([(o_in, o3), (x_in, x), (nscale, v_ns), (bo, v_bo), (b1, v_b1), (b2, v_b2), (bd, v_bd)], small_sem)
    start(early)
    comm.greet()
    stream.prime(0, N_SLOTS_C)
    early[0].wait()
    for h in range(HEADS):
        o_bf[:, 128 * h:128 * (h + 1)] = o3[pl.ds(h, ROWS, stride=HEADS), :].astype(BF)
    comm.meet()
    body.down(ot, WINDOW, 1, o_bf)
    finish(early[1:])
    body.all_reduce(v_bo, None)
    body.norm(5)
    body.mlp(up, down, 2, v_b1, v_b2, v_bd)
    comm.sent(1)


GROUP = 4
N_GROUP = ROWS // GROUP
LAG = 4


def attention_kernel(pos_s, tok, q_in, k_row, v_row, conv, xb, lru, k_cache, v_cache, slot_pos, o_out, conv_out, lru_out, k_out, v_out, slot_out,
                     slots, sems, v_tok, v_conv, v_lru, v_slot, bias, q3, o3, k_new, v_new, small_sem, state_sem, out_sem):
    stream = Stream(slots, sems, N_SLOTS_B)

    def group_rows(j):
        return pl.ds(pl.multiple_of(j * GROUP * WINDOW, GROUP * WINDOW), GROUP * WINDOW)

    ct = stream.add(N_GROUP, lambda j: [(src.at[group_rows(j)], (pl.ds(0, D), part)) for part, src in ((LEFT, k_cache), (RIGHT, v_cache))])
    early = copies([(tok, v_tok), (slot_pos, v_slot), (q_in, q3), (k_row, k_new), (v_row, v_new)], small_sem)
    start(early)
    stream.prime(0, N_SLOTS_B // 2)
    states = copies([(conv.at[:, 1:3], v_conv.at[:, 0:2]), (xb, v_conv.at[:, 2]), (lru, v_lru)], state_sem)
    start(states)
    stream.prime(N_SLOTS_B // 2, N_SLOTS_B)
    finish(early)
    pos = jnp.broadcast_to(v_tok[...], (ROWS, 128)).T
    target = lax.rem(pos, WINDOW)
    lane = lax.broadcasted_iota(jnp.int32, (ROWS, 128), 1)

    @pl.loop(0, WINDOW // 128)
    def _(i):
        now = jnp.where(lane + i * 128 == target, pos, v_slot[:, cols(i, 128)])
        v_slot[:, cols(i, 128)] = now
        age = pos - now
        good = (now >= 0) & (age >= 0) & (age < WINDOW)
        bias[:, cols(i, 128)] = jnp.where(good, 0.0, -jnp.inf)

    results = copies([(v_conv, conv_out), (v_lru, lru_out), (v_slot, slot_out)], state_sem)

    def outputs(j):
        slot = stream.slot_of(ct[0] + j)
        return [pltpu.make_async_copy(slots.at[slot, :, pl.ds(128 * i, 128)], dst.at[group_rows(j)], out_sem.at[slot, i]) for i, dst in enumerate((k_out, v_out))]

    row16 = lax.broadcasted_iota(jnp.int32, (16, 128), 0)
    ahead = ct[0] - LAG + stream.n_slots
    nt = (((1,), (1,)), ((), ()))

    @pl.loop(0, N_GROUP // 2)
    def _(p):
        got = [stream.wait(ct, 2 * p + g) for g in range(2)]
        for g, slot in enumerate(got):
            for r in range(GROUP):
                seq = (2 * p + g) * GROUP + r
                spot = lax.rem(pos_s[seq], WINDOW)
                base = pl.multiple_of(r * WINDOW + lax.div(spot, 16) * 16, 16)
                for i, new in enumerate((k_new, v_new)):
                    here = (slot, pl.ds(base, 16), pl.ds(128 * i, 128))
                    slots[here] = jnp.where(row16 == lax.rem(spot, 16), new[pl.ds(seq, 1), :], f32(slots[here])).astype(BF)
            start(outputs(2 * p + g))

        pairs = [(slot, h) for slot in got for h in range(GROUP // 2)]
        first = 2 * p * GROUP
        scores = []
        for i, (slot, h) in enumerate(pairs):
            q = q3[pl.ds(pl.multiple_of((first + 2 * i) * HEADS, 2 * HEADS), 2 * HEADS), :].astype(BF)
            halves = []
            for e in range(2):
                r = 2 * h + e
                keys = slots[slot, r * WINDOW:(r + 1) * WINDOW, 0:128]
                score = lax.dot_general(q, keys, nt, preferred_element_type=F32)[HEADS * e:HEADS * (e + 1)] * (128 ** -0.5)
                halves.append(score + bias[pl.ds(first + 2 * i + e, 1), :])
            scores.append(jnp.concatenate(halves, axis=0))
        probs = []
        for score in scores:
            e = jnp.exp(score - jnp.max(score, axis=-1, keepdims=True))
            probs.append((e / jnp.sum(e, axis=-1, keepdims=True)).astype(BF))
        for i, (slot, h) in enumerate(pairs):
            halves = []
            for e in range(2):
                r = 2 * h + e
                values = slots[slot, r * WINDOW:(r + 1) * WINDOW, 128:256]
                halves.append(jnp.dot(probs[i], values, preferred_element_type=F32)[HEADS * e:HEADS * (e + 1)])
            o3[pl.ds(pl.multiple_of((first + 2 * i) * HEADS, 2 * HEADS), 2 * HEADS), :] = jnp.concatenate(halves, axis=0)

        @pl.when(2 * p >= LAG)
        def _():
            @pl.when(2 * p == LAG)
            def _():
                finish(states)
                start(results)

            for g in range(2):
                finish(outputs(2 * p + g - LAG))
                stream.issue(ahead + 2 * p + g, ahead + LAG, ahead + N_GROUP)

    last = pltpu.make_async_copy(o3, o_out, small_sem.at[0])
    last.start()
    for j in range(N_GROUP - LAG, N_GROUP):
        finish(outputs(j))
    finish(results)
    last.wait()


ANY = pl.BlockSpec(memory_space=pl.ANY)


def io_specs():
    in_specs = (P('dp', None), P('dp'), P(None, 'dp', None, 'tp'), P(None, 'dp', 'tp'), P('dp', None, None), P('dp', None, None), P('dp', None),
                P(), P(None, None, 'tp'), P(None, 'tp'), P(None, None, 'tp'), P(None, 'tp'), P(None, None, 'tp'), P(None, 'tp'),
                P(None, 'tp', None, None), P(None, 'tp'), P(None, 'tp', None, None), P(None, 'tp'), P(None, 'tp'), P(None, 'tp', None), P(),
                P(None, 'tp'), P(), P(), P('tp', None), P(),
                P(None, None, 'tp'), P(None, 'tp'), P(None, None, 'tp'), P(None, 'tp'), P(None, 'tp', None), P())
    out_specs = (P('dp', None), P(None, 'dp', None, 'tp'), P(None, 'dp', 'tp'), P('dp', None, None), P('dp', None, None), P('dp', None))
    return in_specs, out_specs


def solution(mesh):
    in_specs, out_specs = io_specs()
    shape = jax.ShapeDtypeStruct

    def local_step(x_in, tok_pos, conv_state, lru_state, k_cache, v_cache, slot_pos, norm_scale, rec_wx, rec_bx, rec_wy, rec_by, conv_w, conv_b, gate_wa, gate_ba, gate_wi, gate_bi, a_param, rec_wout, rec_bout, attn_wq, attn_wk, attn_wv, attn_wo, attn_bo, mlp_w1, mlp_b1, mlp_w2, mlp_b2, mlp_wd, mlp_bd):
        tok = tok_pos.reshape(1, ROWS)
        conv_t = jnp.transpose(conv_state, (0, 2, 1, 3))
        vec, vec_f = pltpu.VMEM((2, LOCAL), BF), pltpu.VMEM((2, LOCAL), F32)
        wide, wide_f = pltpu.VMEM((ROWS, LOCAL), BF), pltpu.VMEM((ROWS, LOCAL), F32)
        table, gates, heads = pltpu.VMEM((ROWS, 128), F32), pltpu.VMEM((8, 176, 176), BF), pltpu.VMEM((ROWS * HEADS, 128), F32)
        scale, mlp_b, pos_row, freq = pltpu.VMEM((3, 2, D), BF), pltpu.VMEM((3, 3072), BF), pltpu.VMEM((1, ROWS), jnp.int32), jnp.asarray(FREQ)
        hidden, out_b = pltpu.VMEM((ROWS, 3072), BF), pltpu.VMEM((3, D), BF)
        dma = pltpu.SemaphoreType.DMA
        row, head_rows, branch, state = shape((ROWS, 128), F32), shape((ROWS * HEADS, 128), F32), shape((2, ROWS, LOCAL), BF), shape((2, ROWS, LOCAL), F32)
        x_mid, xb, lru_mid, q_rows, k_row, v_row = pl.pallas_call(
            recurrent_kernel,
            out_shape=[shape((ROWS, D), BF), branch, state, head_rows, row, row],
            in_specs=[ANY] * 28, out_specs=[ANY] * 6,
            scratch_shapes=body_scratch(N_SLOTS_A, 2) + [hidden, table] + COMM_SCRATCH + [
                pos_row, scale, vec, vec, pltpu.VMEM((2, 4, LOCAL), BF), vec, vec, vec, vec_f, pltpu.VMEM((2, D), BF), mlp_b, mlp_b, out_b, pltpu.VMEM((1, 128), F32), dma((N_SMALL,)),
                pltpu.VMEM((3, ROWS, LOCAL), BF), wide_f, gates, gates, wide, table, wide, wide_f, wide_f, wide, pltpu.VMEM((ROWS, 128), jnp.int32),
                heads, table, table, table, table, dma((2, 4)), dma((2, 2)), dma((3,))],
            compiler_params=pltpu.CompilerParams(collective_id=0, has_side_effects=True, vmem_limit_bytes=VMEM_LIMIT),
            name='recurrent_layers',
        )(tok, x_in, conv_t, lru_state, norm_scale, rec_wx, rec_bx, rec_wy, rec_by, conv_w, conv_b, gate_wa, gate_ba, gate_wi, gate_bi, a_param, rec_wout, rec_bout, mlp_w1, mlp_b1, mlp_w2, mlp_b2, mlp_wd, mlp_bd, freq, attn_wq, attn_wk, attn_wv)
        cache = (ROWS * WINDOW, 128)
        o_rows, conv_out, lru_out, k_out, v_out, slot_out = pl.pallas_call(
            attention_kernel,
            out_shape=[head_rows, shape((2, 3, ROWS, LOCAL), BF), state, shape(cache, BF), shape(cache, BF), shape((ROWS, WINDOW), jnp.int32)],
            in_specs=[pl.BlockSpec(memory_space=pltpu.SMEM)] + [ANY] * 10, out_specs=[ANY] * 6,
            scratch_shapes=body_scratch(N_SLOTS_B, 2)[:2] + [
                pos_row, pltpu.VMEM((2, 3, ROWS, LOCAL), BF), pltpu.VMEM((2, ROWS, LOCAL), F32), pltpu.VMEM((ROWS, WINDOW), jnp.int32), pltpu.VMEM((ROWS, WINDOW), F32),
                heads, heads, table, table, dma((5,)), dma((3,)), dma((N_SLOTS_B, 2))],
            compiler_params=pltpu.CompilerParams(vmem_limit_bytes=VMEM_LIMIT),
            name='attention_layer',
        )(tok_pos, tok, q_rows, k_row, v_row, conv_t, xb, lru_mid, k_cache.reshape(cache), v_cache.reshape(cache), slot_pos)
        x_out = pl.pallas_call(
            final_kernel,
            out_shape=shape((ROWS, D), BF),
            in_specs=[ANY] * 11, out_specs=pl.BlockSpec(memory_space=pltpu.VMEM),
            scratch_shapes=body_scratch(N_SLOTS_C, 2)[:3] + [hidden, table] + COMM_SCRATCH + [scale, pltpu.VMEM((D,), BF), mlp_b, mlp_b, out_b, heads, pltpu.VMEM((ROWS, WINDOW), BF), dma((7,))],
            compiler_params=pltpu.CompilerParams(collective_id=1, has_side_effects=True, vmem_limit_bytes=VMEM_LIMIT),
            name='last_mlp',
        )(x_mid, o_rows, norm_scale, attn_bo, attn_wo, mlp_w1, mlp_b1, mlp_w2, mlp_b2, mlp_wd, mlp_bd)
        return (x_out, jnp.transpose(conv_out, (0, 2, 1, 3)), lru_out, k_out.reshape(k_cache.shape), v_out.reshape(v_cache.shape), slot_out)

    return jax.shard_map(local_step, mesh=mesh, in_specs=in_specs, out_specs=out_specs, check_vma=False)
```

```python
import jax
import jax.numpy as jnp
import numpy as np
from jax import lax
from jax.experimental import pallas as pl
from jax.experimental.pallas import tpu as pltpu
from jax.sharding import PartitionSpec as P

ROPE_BASE = 10000.0
NORM_EPS = 1e-6
BF = jnp.bfloat16
F32 = jnp.float32
ROWS = 128
LOCAL = 1408
D = 4096
TILE = 256
CHUNK = 512
N_CHUNK = D // CHUNK
HALF = ROWS // 2
VMEM_LIMIT = 67043328


class Stream:
    def __init__(self, slots, sems, n_slots):
        self.slots, self.sems, self.n_slots = slots, sems, n_slots
        self.phases = []
        self.total = 0

    def add(self, n, *kinds):
        start = self.total
        self.phases.append((start, n, kinds))
        self.total += n
        return start, kinds

    def slot_of(self, t):
        return lax.rem(t, self.n_slots)

    def copies(self, kind, j, slot):
        return [pltpu.make_async_copy(src, self.slots.at[(slot,) + dst], self.sems.at[slot, i]) for i, (src, dst) in enumerate(kind(j))]

    def start_tile(self, kinds, j, slot):
        n = len(kinds)
        if n == 1:
            for c in self.copies(kinds[0], j, slot):
                c.start()
            return
        for which, kind in enumerate(kinds):
            @pl.when(lax.rem(j, n) == which)
            def _(kind=kind):
                for c in self.copies(kind, lax.div(j, n), slot):
                    c.start()

    def issue(self, t, lo, hi):
        for start, n, kinds in self.phases:
            if start + n <= lo or hi <= start:
                continue

            def go(start=start, kinds=kinds):
                self.start_tile(kinds, t - start, self.slot_of(t))

            if start <= lo and hi <= start + n:
                go()
            else:
                pl.when(jnp.logical_and(t >= start, t < start + n))(go)

    def prime(self, lo, hi):
        for start, n, kinds in self.phases:
            first, stop = max(start, lo), min(start + n, hi, self.n_slots)
            if first < stop:
                @pl.loop(first, stop)
                def _(t, start=start, kinds=kinds):
                    self.start_tile(kinds, t - start, self.slot_of(t))

    def wait(self, phase, j):
        start, kinds = phase
        slot = self.slot_of(start + j)
        for c in self.copies(kinds[0], lax.div(j, len(kinds)), slot):
            c.wait()
        return slot


def full(slot_rows):
    return (pl.ds(0, slot_rows), pl.ds(0, TILE))


def columns(ref, layer, rows):
    return lambda j: [(ref.at[layer, :, pl.ds(pl.multiple_of(j * TILE, TILE), TILE)], full(rows))]


def gelu(v):
    return jax.nn.gelu(v, approximate=True)


def f32(v):
    return v.astype(F32)


def cols(k, width=CHUNK):
    return pl.ds(pl.multiple_of(k * width, width), width)


class Comm:
    def __init__(self, part, r1, cs, r2, fin, r3, s1, q1, s2, q2, s3, q3):
        self.part, self.r1, self.cs, self.r2, self.fin, self.r3 = part, r1, cs, r2, fin, r3
        self.s1, self.q1, self.s2, self.q2, self.s3, self.q3 = s1, q1, s2, q2, s3, q3
        me = lax.axis_index('tp')
        self.mine = lax.rem(me, 2)
        self.other = 1 - self.mine
        self.partner = me + 1 - 2 * self.mine
        self.peer = lax.rem(me + 2, 4)

    def greet(self):
        for dev in (self.partner, self.peer):
            pl.semaphore_signal(pltpu.get_barrier_semaphore(), inc=1, device_id={'tp': dev}, device_id_type=pl.DeviceIdType.MESH)

    def meet(self):
        pl.semaphore_wait(pltpu.get_barrier_semaphore(), 2)

    def copy1(self, par, k):
        return pltpu.make_async_remote_copy(src_ref=self.part.at[k, self.other], dst_ref=self.r1.at[k], send_sem=self.s1.at[par, k], recv_sem=self.q1.at[par, k], device_id={'tp': self.partner}, device_id_type=pl.DeviceIdType.MESH)

    def copy2(self, par, k):
        return pltpu.make_async_remote_copy(src_ref=self.cs.at[k], dst_ref=self.r2.at[par, k], send_sem=self.s2.at[par, k], recv_sem=self.q2.at[par, k], device_id={'tp': self.peer}, device_id_type=pl.DeviceIdType.MESH)

    def copy3(self, par, k):
        return pltpu.make_async_remote_copy(src_ref=self.fin.at[k], dst_ref=self.r3.at[k], send_sem=self.s3.at[par, k], recv_sem=self.q3.at[par, k], device_id={'tp': self.partner}, device_id_type=pl.DeviceIdType.MESH)

    def chip_sum(self, par, k):
        self.copy1(par, k).wait_recv()
        self.cs[k] = (f32(self.part[k, self.mine]) + f32(self.r1[k])).astype(BF)
        self.copy2(par, k).start()

    def finish(self, par, update):
        @pl.loop(0, N_CHUNK)
        def _(k):
            self.copy2(par, k).wait_recv()
            total = (f32(self.cs[k]) + f32(self.r2[par, k])).astype(BF)
            self.fin[k] = total
            self.copy3(par, k).start()
            update(self.mine, k, f32(total))

            @pl.when(k >= 1)
            def _():
                self.copy3(par, k - 1).wait_recv()
                update(self.other, k - 1, f32(self.r3[k - 1]))

        self.copy3(par, N_CHUNK - 1).wait_recv()
        update(self.other, N_CHUNK - 1, f32(self.r3[N_CHUNK - 1]))

    def sent(self, par):
        @pl.loop(0, N_CHUNK)
        def _(k):
            self.copy1(par, k).wait_send()
            self.copy2(par, k).wait_send()
            self.copy3(par, k).wait_send()


def fold_lanes(v):
    acc = v[:, 0:128]
    for i in range(1, v.shape[1] // 128):
        acc = acc + v[:, 128 * i:128 * (i + 1)]
    return acc


class Body:
    def __init__(self, stream, comm, x, n, hid, ss, nscale):
        self.stream, self.comm, self.x, self.n, self.hid, self.ss, self.nscale = stream, comm, x, n, hid, ss, nscale
        self.n_ar = 0

    def squares(self):
        self.ss[...] = jnp.zeros_like(self.ss)

        @pl.loop(0, N_CHUNK)
        def _(k):
            v = f32(self.x[:, cols(k)])
            self.ss[...] += fold_lanes(v * v)

    def norm(self, row):
        scale = lax.rsqrt(jnp.sum(self.ss[...], axis=-1, keepdims=True) * (1.0 / D) + NORM_EPS)

        @pl.loop(0, N_CHUNK)
        def _(k):
            gain = 1.0 + f32(self.nscale[row // 2, row % 2:row % 2 + 1, cols(k)])
            self.n[:, cols(k)] = (f32(self.x[:, cols(k)]) * scale * gain).astype(BF)

        if self.n_ar:
            self.comm.sent((self.n_ar - 1) % 2)

    def updater(self, bias, row):
        def update(half, k, u):
            rows = pl.ds(pl.multiple_of(half * HALF, HALF), HALF)
            new = (f32(self.x[rows, cols(k)]) + u + f32(bias[cols(k)].reshape(1, CHUNK) if row is None else bias[row:row + 1, cols(k)])).astype(BF)
            self.x[rows, cols(k)] = new
            v = f32(new)
            self.ss[rows, :] += fold_lanes(v * v)

        return update

    def all_reduce(self, bias, row):
        par = self.n_ar % 2
        self.n_ar += 1
        self.ss[...] = jnp.zeros_like(self.ss)
        self.comm.finish(par, self.updater(bias, row))

    def down(self, phase, depth, per_chunk, lhs):
        st, comm, par = self.stream, self.comm, self.n_ar % 2
        start = phase[0]
        ahead = start + st.n_slots
        stop = ahead + per_chunk * N_CHUNK

        @pl.loop(0, N_CHUNK)
        def _(k):
            for h in range(2):
                if per_chunk == 2 or h == 0:
                    slot = st.wait(phase, k * per_chunk + h)
                off = 0 if per_chunk == 2 else h * depth
                prod = jnp.dot(lhs[...], st.slots[slot, off:off + depth, :], preferred_element_type=F32).astype(BF)
                for r in range(2):
                    comm.part[k, r, :, h * TILE:(h + 1) * TILE] = prod[r * HALF:(r + 1) * HALF]
            for h in range(per_chunk):
                st.issue(ahead + k * per_chunk + h, ahead, stop)
            comm.copy1(par, k).start()

            @pl.when(k >= 1)
            def _():
                comm.chip_sum(par, k - 1)

        comm.chip_sum(par, N_CHUNK - 1)

    def mlp(self, up, down, layer, b1, b2, bd):
        st = self.stream
        start = up[0]
        ahead = start + st.n_slots
        stop = ahead + 24

        @pl.loop(0, 6)
        def _(q):
            got = [st.wait(up, 4 * q + h) for h in range(4)]
            dots = [jnp.dot(self.n[...], st.slots[slot], preferred_element_type=F32) for slot in got]
            for h in range(4):
                st.issue(ahead + 4 * q + h, ahead, stop)
            for h in range(2):
                c = cols(2 * q + h, TILE)
                gate = dots[2 * h] + f32(b1[layer:layer + 1, c])
                lin = dots[2 * h + 1] + f32(b2[layer:layer + 1, c])
                self.hid[:, c] = (gelu(gate) * lin).astype(BF)

        self.down(down, 3072, 2, self.hid)
        self.all_reduce(bd, layer)


    def recurrent(self, x_tiles, mixed, y_tiles, out_tiles, layer, v, outs):
        st = self.stream
        ahead = x_tiles[0] + st.n_slots
        stop = ahead + 11

        def dots(phase, tiles):
            slots = [st.wait(phase, i) for i in tiles]
            return [jnp.dot(self.n[...], st.slots[slot], preferred_element_type=F32) for slot in slots]

        def put_x(i, g):
            v.xb[:, cols(i, TILE)] = (g + f32(v.bx[layer:layer + 1, cols(i, TILE)])).astype(BF)

        @pl.loop(0, 2)
        def _(p):
            for h, g in enumerate(dots(x_tiles, [2 * p, 2 * p + 1])):
                put_x(2 * p + h, g)
            for h in range(2):
                st.issue(ahead + 2 * p + h, ahead, stop)

        outs.wait_inputs(layer)
        pos = v.tokc[...]

        def conv(i):
            c = slice(128 * i, 128 * (i + 1))
            acc = f32(v.cb[layer:layer + 1, c]) + f32(v.cw[layer, 0:1, c]) * f32(v.xb[:, c])
            for j in range(3):
                acc = acc + jnp.where(pos >= 3 - j, f32(v.conv[j, :, c]), 0.0) * f32(v.cw[layer, 3 - j:4 - j, c])
            v.xc[:, c] = acc.astype(BF)

        if layer == 0:
            self.comm.meet()
        slots = [st.wait(x_tiles, 4), st.wait(mixed, 0)]
        last_x, g = [jnp.dot(self.n[...], st.slots[slot], preferred_element_type=F32) for slot in slots]
        for i in range(8):
            conv(i)
        put_x(4, last_x)
        v.xb[:, 1280:] = (g[:, :128] + f32(v.bx[layer:layer + 1, 1280:])).astype(BF)
        v.yg[...] = gelu(g[:, 128:] + f32(v.by[layer:layer + 1, 1280:]))
        for h in range(2):
            st.issue(ahead + 4 + h, ahead, stop)

        first_y, = dots(y_tiles, [0])
        for i in range(8, 11):
            conv(i)
        for b in range(8):
            c = slice(176 * b, 176 * (b + 1))
            xc = v.xc[:, c]
            v.rp[:, c] = jnp.dot(xc, v.ga[b], preferred_element_type=F32)
            v.ip[:, c] = jnp.dot(xc, v.gi[b], preferred_element_type=F32)

        def gate(c, reset):
            rate = -8.0 * jax.nn.softplus(v.ap[layer:layer + 1, c])
            decay = jnp.exp(rate * jax.nn.sigmoid(v.rp[:, c] + f32(v.gba[layer:layer + 1, c])))
            into = jnp.sqrt(1.0 - decay * decay)
            decay = jnp.where(reset, 0.0, decay)
            into = jnp.where(reset, 1.0, into)
            new = decay * v.lru[:, c] + into * jax.nn.sigmoid(v.ip[:, c] + f32(v.gbi[layer:layer + 1, c])) * f32(v.xc[:, c])
            v.lru[:, c] = new
            return new

        def put_y(i, g):
            for h in range(2):
                c = cols(2 * i + h, 128)
                new = gate(c, pos == 0)
                y = gelu(g[:, 128 * h:128 * (h + 1)] + f32(v.by[layer:layer + 1, c]))
                v.gated[:, c] = (new * y).astype(BF)

        put_y(0, first_y)
        st.issue(ahead + 6, ahead, stop)

        @pl.loop(0, 2)
        def _(p):
            for h, g in enumerate(dots(y_tiles, [2 * p + 1, 2 * p + 2])):
                put_y(2 * p + 1 + h, g)
            for h in range(2):
                st.issue(ahead + 7 + 2 * p + h, ahead, stop)

        c = slice(1280, 1408)
        v.gated[:, c] = (gate(c, pos == 0) * v.yg[...]).astype(BF)
        outs.write(layer)
        self.down(out_tiles, 1408, 1, v.gated)
        self.all_reduce(v.bout, layer)
        outs.wait_write(layer)
        if layer == 0:
            outs.start_inputs(1)


def add_mlp(stream, w1, w2, wd, layer):
    up = stream.add(24, columns(w1, layer, D), columns(w2, layer, D))
    return up, stream.add(16, columns(wd, layer, 3072))


class Names:
    def __init__(self, **kw):
        self.__dict__.update(kw)


class StateCopies:
    def __init__(self, ins, xb_out, lru_out, v, in_sem, out_sem):
        self.ins, self.xb_out, self.lru_out, self.v, self.in_sem, self.out_sem = ins, xb_out, lru_out, v, in_sem, out_sem

    def inputs(self, layer):
        return [pltpu.make_async_copy(src.at[layer], dst, self.in_sem.at[layer, i]) for i, (src, dst) in enumerate(self.ins)]

    def start_inputs(self, layer):
        for c in self.inputs(layer):
            c.start()

    def wait_inputs(self, layer):
        for c in self.inputs(layer):
            c.wait()

    def outputs(self, layer):
        pairs = [(self.v.xb, self.xb_out.at[layer]), (self.v.lru, self.lru_out.at[layer])]
        return [pltpu.make_async_copy(src, dst, self.out_sem.at[layer, i]) for i, (src, dst) in enumerate(pairs)]

    def write(self, layer):
        for c in self.outputs(layer):
            c.start()

    def wait_write(self, layer):
        for c in self.outputs(layer):
            c.wait()


N_SLOTS_A = 19
WINDOW = 1024
HEADS = 8
N_COMM = 12
N_SMALL = 15
LEFT = pl.ds(0, 128)
RIGHT = pl.ds(128, 128)
FREQ = np.zeros((1, 128), np.float32)
FREQ[0, :32] = FREQ[0, 32:64] = np.float32(ROPE_BASE) ** (-np.arange(32, dtype=np.float32) / 32)


def copies(pairs, sem):
    return [pltpu.make_async_copy(a, b, sem.at[i]) for i, (a, b) in enumerate(pairs)]


def start(group):
    for c in group:
        c.start()


def finish(group):
    for c in group:
        c.wait()


N_SLOTS_B = 25
N_SLOTS_C = 23

COMM_SCRATCH = [
    pltpu.VMEM((N_CHUNK, 2, HALF, CHUNK), BF), pltpu.VMEM((N_CHUNK, HALF, CHUNK), BF), pltpu.VMEM((N_CHUNK, HALF, CHUNK), BF),
    pltpu.VMEM((2, N_CHUNK, HALF, CHUNK), BF), pltpu.VMEM((N_CHUNK, HALF, CHUNK), BF), pltpu.VMEM((N_CHUNK, HALF, CHUNK), BF),
] + [pltpu.SemaphoreType.DMA((2, N_CHUNK)) for _ in range(6)]


def body_scratch(n_slots, n_pieces):
    return [pltpu.VMEM((n_slots, D, TILE), BF), pltpu.SemaphoreType.DMA((n_slots, n_pieces)), pltpu.VMEM((ROWS, D), BF), pltpu.VMEM((ROWS, D), BF)]


def recurrent_kernel(tok, x_in, conv, lru, nscale, wx, bx, wy, by, cw, cb, ga, gba, gi, gbi, ap, wout, bout, w1, b1, w2, b2, wd, bd, freq, wq, wk, wv, *refs):
    (x_out, xb_out, lru_out, q_out, k_row, v_row), refs = refs[:6], refs[6:]
    (slots, sems, x, n, hid, ss), refs = refs[:6], refs[6:]
    comm = Comm(*refs[:N_COMM])
    refs = refs[N_COMM:]
    small, refs = refs[:N_SMALL], refs[N_SMALL:]
    v_tok, v_ns, v_bx, v_by, v_cw, v_cb, v_gba, v_gbi, v_ap, v_bout, v_b1, v_b2, v_bd, v_freq, small_sem = small
    v_conv, v_lru, v_ga, v_gi, xb, yg, xc, rp, ip, gated, tokc, q3, k_new, v_new, v_cos, v_sin, in_sem, out_sem, row_sem = refs
    stream = Stream(slots, sems, N_SLOTS_A)
    v = Names(bx=v_bx, by=v_by, cw=v_cw, cb=v_cb, ga=v_ga, gba=v_gba, gi=v_gi, gbi=v_gbi, ap=v_ap, bout=v_bout, conv=v_conv, lru=v_lru, xb=xb, yg=yg, xc=xc, rp=rp, ip=ip, gated=gated, tokc=tokc)
    outs = StateCopies([(conv, v_conv), (lru, v_lru), (ga, v_ga), (gi, v_gi)], xb_out, lru_out, v, in_sem, out_sem)
    body = Body(stream, comm, x, n, hid, ss, v_ns)

    plan = []
    for layer in range(2):
        xt = stream.add(5, columns(wx, layer, D))
        mixed = stream.add(1, lambda j, layer=layer: [(wx.at[layer, :, 1280:1408], (pl.ds(0, D), pl.ds(0, 128))), (wy.at[layer, :, 1280:1408], (pl.ds(0, D), pl.ds(128, 128)))])
        yt = stream.add(5, columns(wy, layer, D))
        ot = stream.add(8, lambda j, layer=layer: [(wout.at[layer, :, pl.ds(pl.multiple_of(j * CHUNK + h * TILE, TILE), TILE)], (pl.ds(h * 1408, 1408), pl.ds(0, TILE))) for h in range(2)])
        up, down = add_mlp(stream, w1, w2, wd, layer)
        plan.append((xt, mixed, yt, ot, up, down))
    qt = stream.add(4, lambda j: [(wq.at[:, cols(j, TILE)], full(D))])
    kvt = stream.add(1, lambda j: [(wk, (pl.ds(0, D), LEFT)), (wv, (pl.ds(0, D), RIGHT))])

    pairs = [(x_in, x), (tok, v_tok), (nscale, v_ns), (bx, v_bx), (by, v_by), (cw, v_cw), (cb, v_cb), (gba, v_gba), (gbi, v_gbi), (ap, v_ap), (bout, v_bout), (b1, v_b1), (b2, v_b2), (bd, v_bd), (freq, v_freq)]
    early = copies(pairs, small_sem)
    start(early)
    comm.greet()
    stream.prime(0, 6)
    outs.start_inputs(0)
    stream.prime(6, N_SLOTS_A)
    for c in early:
        c.wait()
    tokc[...] = jnp.broadcast_to(v_tok[...], (ROWS, 128)).T
    body.squares()
    for layer in range(2):
        xt, mixed, yt, ot, up, down = plan[layer]
        body.norm(2 * layer)
        body.recurrent(xt, mixed, yt, ot, layer, v, outs)
        body.norm(2 * layer + 1)
        body.mlp(up, down, layer, v_b1, v_b2, v_bd)
    last = pltpu.make_async_copy(x, x_out, small_sem.at[0])
    last.start()
    body.norm(4)
    lane = lax.broadcasted_iota(jnp.int32, (ROWS, 128), 1)
    angle = f32(tokc[...]) * v_freq[...]
    v_cos[...] = jnp.cos(angle)
    v_sin[...] = jnp.sin(angle) * jnp.where(lane < 32, -1.0, 1.0)

    def rope(val):
        other = jnp.where(lane < 32, pltpu.roll(val, 96, 1), pltpu.roll(val, 32, 1))
        return f32((val * v_cos[...] + other * v_sin[...]).astype(BF))

    @pl.loop(0, 2)
    def _(p):
        got = [stream.wait(qt, 2 * p + i) for i in range(2)]
        for i, slot in enumerate(got):
            g = jnp.dot(n[...], slots[slot], preferred_element_type=F32)
            for h in range(2):
                q3[pl.ds(4 * p + 2 * i + h, ROWS, stride=HEADS), :] = rope(g[:, 128 * h:128 * (h + 1)])

    slot = stream.wait(kvt, 0)
    g = jnp.dot(n[...], slots[slot], preferred_element_type=F32)
    k_new[...] = rope(g[:, :128])
    v_new[...] = f32(g[:, 128:].astype(BF))
    rows = copies([(q3, q_out), (k_new, k_row), (v_new, v_row)], row_sem)
    start(rows)
    finish(rows)
    last.wait()


def final_kernel(x_in, o_in, nscale, bo, wo, w1, b1, w2, b2, wd, bd, *refs):
    (x, slots, sems, n, hid, ss), refs = refs[:6], refs[6:]
    comm = Comm(*refs[:N_COMM])
    v_ns, v_bo, v_b1, v_b2, v_bd, o3, o_bf, small_sem = refs[N_COMM:]
    stream = Stream(slots, sems, N_SLOTS_C)
    body = Body(stream, comm, x, n, hid, ss, v_ns)
    ot = stream.add(8, lambda j: [(wo.at[:, pl.ds(pl.multiple_of(j * CHUNK + h * TILE, TILE), TILE)], (pl.ds(h * WINDOW, WINDOW), pl.ds(0, TILE))) for h in range(2)])
    up, down = add_mlp(stream, w1, w2, wd, 2)
    early = copies([(o_in, o3), (x_in, x), (nscale, v_ns), (bo, v_bo), (b1, v_b1), (b2, v_b2), (bd, v_bd)], small_sem)
    start(early)
    comm.greet()
    stream.prime(0, N_SLOTS_C)
    early[0].wait()
    for h in range(HEADS):
        o_bf[:, 128 * h:128 * (h + 1)] = o3[pl.ds(h, ROWS, stride=HEADS), :].astype(BF)
    comm.meet()
    body.down(ot, WINDOW, 1, o_bf)
    finish(early[1:])
    body.all_reduce(v_bo, None)
    body.norm(5)
    body.mlp(up, down, 2, v_b1, v_b2, v_bd)
    comm.sent(1)


GROUP = 4
N_GROUP = ROWS // GROUP
LAG = 8


def attention_kernel(pos_s, tok, q_in, k_row, v_row, conv, xb, lru, k_cache, v_cache, slot_pos, o_out, conv_out, lru_out, k_out, v_out, slot_out,
                     slots, sems, v_tok, v_conv, v_lru, v_slot, bias, q3, o3, k_new, v_new, small_sem, state_sem, out_sem):
    stream = Stream(slots, sems, N_SLOTS_B)

    def group_rows(j):
        return pl.ds(pl.multiple_of(j * GROUP * WINDOW, GROUP * WINDOW), GROUP * WINDOW)

    ct = stream.add(N_GROUP, lambda j: [(src.at[group_rows(j)], (pl.ds(0, D), part)) for part, src in ((LEFT, k_cache), (RIGHT, v_cache))])
    early = copies([(tok, v_tok), (slot_pos, v_slot), (q_in, q3), (k_row, k_new), (v_row, v_new)], small_sem)
    start(early)
    stream.prime(0, N_SLOTS_B // 2)
    states = copies([(conv.at[:, 1:3], v_conv.at[:, 0:2]), (xb, v_conv.at[:, 2]), (lru, v_lru)], state_sem)
    start(states)
    stream.prime(N_SLOTS_B // 2, N_SLOTS_B)
    finish(early)
    pos = jnp.broadcast_to(v_tok[...], (ROWS, 128)).T
    target = lax.rem(pos, WINDOW)
    lane = lax.broadcasted_iota(jnp.int32, (ROWS, 128), 1)

    @pl.loop(0, WINDOW // 128)
    def _(i):
        now = jnp.where(lane + i * 128 == target, pos, v_slot[:, cols(i, 128)])
        v_slot[:, cols(i, 128)] = now
        age = pos - now
        good = (now >= 0) & (age >= 0) & (age < WINDOW)
        bias[:, cols(i, 128)] = jnp.where(good, 0.0, -jnp.inf)

    results = copies([(v_conv, conv_out), (v_lru, lru_out), (v_slot, slot_out)], state_sem)

    def outputs(j):
        slot = stream.slot_of(ct[0] + j)
        return [pltpu.make_async_copy(slots.at[slot, :, pl.ds(128 * i, 128)], dst.at[group_rows(j)], out_sem.at[slot, i]) for i, dst in enumerate((k_out, v_out))]

    row16 = lax.broadcasted_iota(jnp.int32, (16, 128), 0)
    ahead = ct[0] - LAG + stream.n_slots
    nt = (((1,), (1,)), ((), ()))

    @pl.loop(0, N_GROUP // 2)
    def _(p):
        got = [stream.wait(ct, 2 * p + g) for g in range(2)]
        for g, slot in enumerate(got):
            for r in range(GROUP):
                seq = (2 * p + g) * GROUP + r
                spot = lax.rem(pos_s[seq], WINDOW)
                base = pl.multiple_of(r * WINDOW + lax.div(spot, 16) * 16, 16)
                for i, new in enumerate((k_new, v_new)):
                    here = (slot, pl.ds(base, 16), pl.ds(128 * i, 128))
                    slots[here] = jnp.where(row16 == lax.rem(spot, 16), new[pl.ds(seq, 1), :], f32(slots[here])).astype(BF)
            start(outputs(2 * p + g))

        pairs = [(slot, h) for slot in got for h in range(GROUP // 2)]
        first = 2 * p * GROUP
        scores = []
        for i, (slot, h) in enumerate(pairs):
            q = q3[pl.ds(pl.multiple_of((first + 2 * i) * HEADS, 2 * HEADS), 2 * HEADS), :].astype(BF)
            halves = []
            for e in range(2):
                r = 2 * h + e
                keys = slots[slot, r * WINDOW:(r + 1) * WINDOW, 0:128]
                score = lax.dot_general(q, keys, nt, preferred_element_type=F32)[HEADS * e:HEADS * (e + 1)] * (128 ** -0.5)
                halves.append(score + bias[pl.ds(first + 2 * i + e, 1), :])
            scores.append(jnp.concatenate(halves, axis=0))
        probs = []
        for score in scores:
            e = jnp.exp(score - jnp.max(score, axis=-1, keepdims=True))
            probs.append((e / jnp.sum(e, axis=-1, keepdims=True)).astype(BF))
        for i, (slot, h) in enumerate(pairs):
            halves = []
            for e in range(2):
                r = 2 * h + e
                values = slots[slot, r * WINDOW:(r + 1) * WINDOW, 128:256]
                halves.append(jnp.dot(probs[i], values, preferred_element_type=F32)[HEADS * e:HEADS * (e + 1)])
            o3[pl.ds(pl.multiple_of((first + 2 * i) * HEADS, 2 * HEADS), 2 * HEADS), :] = jnp.concatenate(halves, axis=0)

        @pl.when(2 * p >= LAG)
        def _():
            @pl.when(2 * p == LAG)
            def _():
                finish(states)
                start(results)

            for g in range(2):
                finish(outputs(2 * p + g - LAG))
                stream.issue(ahead + 2 * p + g, ahead + LAG, ahead + N_GROUP)

    last = pltpu.make_async_copy(o3, o_out, small_sem.at[0])
    last.start()
    for j in range(N_GROUP - LAG, N_GROUP):
        finish(outputs(j))
    finish(results)
    last.wait()


ANY = pl.BlockSpec(memory_space=pl.ANY)


def io_specs():
    in_specs = (P('dp', None), P('dp'), P(None, 'dp', None, 'tp'), P(None, 'dp', 'tp'), P('dp', None, None), P('dp', None, None), P('dp', None),
                P(), P(None, None, 'tp'), P(None, 'tp'), P(None, None, 'tp'), P(None, 'tp'), P(None, None, 'tp'), P(None, 'tp'),
                P(None, 'tp', None, None), P(None, 'tp'), P(None, 'tp', None, None), P(None, 'tp'), P(None, 'tp'), P(None, 'tp', None), P(),
                P(None, 'tp'), P(), P(), P('tp', None), P(),
                P(None, None, 'tp'), P(None, 'tp'), P(None, None, 'tp'), P(None, 'tp'), P(None, 'tp', None), P())
    out_specs = (P('dp', None), P(None, 'dp', None, 'tp'), P(None, 'dp', 'tp'), P('dp', None, None), P('dp', None, None), P('dp', None))
    return in_specs, out_specs


def solution(mesh):
    in_specs, out_specs = io_specs()
    shape = jax.ShapeDtypeStruct

    def local_step(x_in, tok_pos, conv_state, lru_state, k_cache, v_cache, slot_pos, norm_scale, rec_wx, rec_bx, rec_wy, rec_by, conv_w, conv_b, gate_wa, gate_ba, gate_wi, gate_bi, a_param, rec_wout, rec_bout, attn_wq, attn_wk, attn_wv, attn_wo, attn_bo, mlp_w1, mlp_b1, mlp_w2, mlp_b2, mlp_wd, mlp_bd):
        tok = tok_pos.reshape(1, ROWS)
        conv_t = jnp.transpose(conv_state, (0, 2, 1, 3))
        vec, vec_f = pltpu.VMEM((2, LOCAL), BF), pltpu.VMEM((2, LOCAL), F32)
        wide, wide_f = pltpu.VMEM((ROWS, LOCAL), BF), pltpu.VMEM((ROWS, LOCAL), F32)
        table, gates, heads = pltpu.VMEM((ROWS, 128), F32), pltpu.VMEM((8, 176, 176), BF), pltpu.VMEM((ROWS * HEADS, 128), F32)
        scale, mlp_b, pos_row, freq = pltpu.VMEM((3, 2, D), BF), pltpu.VMEM((3, 3072), BF), pltpu.VMEM((1, ROWS), jnp.int32), jnp.asarray(FREQ)
        hidden, out_b = pltpu.VMEM((ROWS, 3072), BF), pltpu.VMEM((3, D), BF)
        dma = pltpu.SemaphoreType.DMA
        row, head_rows, branch, state = shape((ROWS, 128), F32), shape((ROWS * HEADS, 128), F32), shape((2, ROWS, LOCAL), BF), shape((2, ROWS, LOCAL), F32)
        x_mid, xb, lru_mid, q_rows, k_row, v_row = pl.pallas_call(
            recurrent_kernel,
            out_shape=[shape((ROWS, D), BF), branch, state, head_rows, row, row],
            in_specs=[ANY] * 28, out_specs=[ANY] * 6,
            scratch_shapes=body_scratch(N_SLOTS_A, 2) + [hidden, table] + COMM_SCRATCH + [
                pos_row, scale, vec, vec, pltpu.VMEM((2, 4, LOCAL), BF), vec, vec, vec, vec_f, pltpu.VMEM((2, D), BF), mlp_b, mlp_b, out_b, pltpu.VMEM((1, 128), F32), dma((N_SMALL,)),
                pltpu.VMEM((3, ROWS, LOCAL), BF), wide_f, gates, gates, wide, table, wide, wide_f, wide_f, wide, pltpu.VMEM((ROWS, 128), jnp.int32),
                heads, table, table, table, table, dma((2, 4)), dma((2, 2)), dma((3,))],
            compiler_params=pltpu.CompilerParams(collective_id=0, has_side_effects=True, vmem_limit_bytes=VMEM_LIMIT),
            name='recurrent_layers',
        )(tok, x_in, conv_t, lru_state, norm_scale, rec_wx, rec_bx, rec_wy, rec_by, conv_w, conv_b, gate_wa, gate_ba, gate_wi, gate_bi, a_param, rec_wout, rec_bout, mlp_w1, mlp_b1, mlp_w2, mlp_b2, mlp_wd, mlp_bd, freq, attn_wq, attn_wk, attn_wv)
        cache = (ROWS * WINDOW, 128)
        o_rows, conv_out, lru_out, k_out, v_out, slot_out = pl.pallas_call(
            attention_kernel,
            out_shape=[head_rows, shape((2, 3, ROWS, LOCAL), BF), state, shape(cache, BF), shape(cache, BF), shape((ROWS, WINDOW), jnp.int32)],
            in_specs=[pl.BlockSpec(memory_space=pltpu.SMEM)] + [ANY] * 10, out_specs=[ANY] * 6,
            scratch_shapes=body_scratch(N_SLOTS_B, 2)[:2] + [
                pos_row, pltpu.VMEM((2, 3, ROWS, LOCAL), BF), pltpu.VMEM((2, ROWS, LOCAL), F32), pltpu.VMEM((ROWS, WINDOW), jnp.int32), pltpu.VMEM((ROWS, WINDOW), F32),
                heads, heads, table, table, dma((5,)), dma((3,)), dma((N_SLOTS_B, 2))],
            compiler_params=pltpu.CompilerParams(vmem_limit_bytes=VMEM_LIMIT),
            name='attention_layer',
        )(tok_pos, tok, q_rows, k_row, v_row, conv_t, xb, lru_mid, k_cache.reshape(cache), v_cache.reshape(cache), slot_pos)
        x_out = pl.pallas_call(
            final_kernel,
            out_shape=shape((ROWS, D), BF),
            in_specs=[ANY] * 11, out_specs=pl.BlockSpec(memory_space=pltpu.VMEM),
            scratch_shapes=body_scratch(N_SLOTS_C, 2)[:3] + [hidden, table] + COMM_SCRATCH + [scale, pltpu.VMEM((D,), BF), mlp_b, mlp_b, out_b, heads, pltpu.VMEM((ROWS, WINDOW), BF), dma((7,))],
            compiler_params=pltpu.CompilerParams(collective_id=1, has_side_effects=True, vmem_limit_bytes=VMEM_LIMIT),
            name='last_mlp',
        )(x_mid, o_rows, norm_scale, attn_bo, attn_wo, mlp_w1, mlp_b1, mlp_w2, mlp_b2, mlp_wd, mlp_bd)
        return (x_out, jnp.transpose(conv_out, (0, 2, 1, 3)), lru_out, k_out.reshape(k_cache.shape), v_out.reshape(v_cache.shape), slot_out)

    return jax.shard_map(local_step, mesh=mesh, in_specs=in_specs, out_specs=out_specs, check_vma=False)
```
